128 devices in a mesh: row: 8 (over x, core), col: 16 (over z, y).
Axes of the slice: x: 4, y: 4, z: 4, core: 2. Of those that a mesh axis runs over, the one named last changes fastest.
Arguments:
- matrix: float32 [8192, 8192], P('row', 'col'), as said below
- start_vectors: float32 [8192, 512], P(('col', 'row')), may hold values from -6 to 6
- interval: float32 [2], replicated, as said below
Outputs:
- ortho_basis: float32 [8192, 512], P(('col', 'row'))
- projected: float32 [512, 512], replicated
- residual: float32 [8192, 512], P(('col', 'row'))
The draws below stay inside these ranges and needn't reach their ends.
Inputs may be any that keep to these rules, and one draw needn't show every extreme that they name: matrix is exactly symmetric (entry (r, c) equals entry (c, r)); its eigenvalues lie within about -1.45 to 1.45. interval[0] lies in [-1.2, -0.7] and interval[1] in [1.45, 1.9].
All inputs are finite; a program needn't handle non-finite values.
Results may differ from the reference program's by a relative error of at most 0.0003.
Values sent between devices are 32-bit elements.
No kernel may reach another device: no remote copies, remote signals or barrier semaphores. Data moves between devices by JAX's collectives and lax.ppermute only.
A program may use at most 128 MiB of HBM per device.

```python
import math
import jax
import jax.numpy as jnp
from jax import lax

K = 512
FILTER_DEG = 3
OUTER = 2
N = 8192


def draw_matrix(key, part):
    entries = jax.random.normal(key, (N, N), jnp.float32)
    return ((entries + entries.T) * (0.5 / math.sqrt(N))).astype(jnp.float32)


def draw_interval(key, part):
    low_key = jax.random.fold_in(key, 11)
    high_key = jax.random.fold_in(key, 23)
    low_end = jax.random.uniform(low_key, (), jnp.float32, -1.2, -0.7)
    high_end = jax.random.uniform(high_key, (), jnp.float32, 1.45, 1.9)
    return jnp.stack([low_end, high_end]).astype(jnp.float32)


def shard_levels(rng, extent, split, least, high):
    def one(axis_at, blocks):
        steps = jax.random.uniform(jax.random.fold_in(jax.random.fold_in(rng, 6), axis_at), (blocks,), jnp.float32, least / len(split), high / len(split))
        return jnp.repeat(jnp.exp(steps), extent[axis_at] // blocks).reshape((-1,) + (1,) * (len(extent) - axis_at - 1))

    gain = one(*split[0])
    for cut in split[1:]:
        gain = gain * one(*cut)
    return gain


def gaussian(rng, extent, deviation, limit, cuts=(), kind=jnp.bfloat16):
    values = jax.random.normal(rng, extent, jnp.float32) * deviation
    if len(cuts) > 0:
        values = shard_levels(rng, extent, cuts, -0.22, 0.18) * values
    return jnp.clip(values, min=-limit, max=limit).astype(kind)


def setup_inputs(seed: int = 0) -> dict:
    keys = jax.random.split(jax.random.key(seed), 4)
    matrix = draw_matrix(jax.random.fold_in(keys[3], 71), 0)
    start_vectors = gaussian(keys[1], (N, K), 1.0, 6.0, ((0, 128),), jnp.float32)
    interval = draw_interval(jax.random.fold_in(keys[3], 71), 0)
    return dict(matrix=matrix, start_vectors=start_vectors, interval=interval)


def product(left, right):
    return jnp.dot(left, right, precision=lax.Precision.HIGHEST, preferred_element_type=jnp.float32)


def tri_solve(factor, values):
    return jax.scipy.linalg.solve_triangular(factor, values, lower=True)


def reference(matrix, start_vectors, interval):
    center = 0.5 * (interval[0] + interval[1])
    half_width = 0.5 * (interval[1] - interval[0])
    total_rows = matrix.shape[0]
    positions = lax.iota(jnp.int32, total_rows)
    diagonal = positions[:, None] == positions[None, :]
    operator = jnp.where(diagonal, matrix - center, matrix) / half_width
    current_start = start_vectors
    for sweep_index in range(OUTER):
        previous = current_start
        current = product(operator, current_start)
        for degree in range(2, FILTER_DEG + 1):
            previous, current = current, 2.0 * product(operator, current) - previous
        mapped = product(operator, current)
        gram_matrix = product(current.T, current) / total_rows
        cross_terms = product(current.T, mapped) / total_rows
        factor = jnp.linalg.cholesky(gram_matrix)
        ortho_basis = tri_solve(factor, current.T).T
        partial_value = tri_solve(factor, cross_terms)
        projected = tri_solve(factor, partial_value.T).T
        current_start = ortho_basis
    residual = tri_solve(factor, mapped.T).T - product(ortho_basis, projected)
    return ortho_basis, projected, residual
```

```python
import functools

import jax
import jax.numpy as jnp
from jax import lax
from jax.experimental import pallas as pl
from jax.experimental.pallas import tpu as pltpu
from jax.sharding import Mesh
from jax.sharding import PartitionSpec as P


ALL = ("x", "k", "z", "y")
ROW = ("x", "k")
COL = ("z", "y")
HIGHEST = lax.Precision.HIGHEST


def dot(left, right, left_dim=1, right_dim=0):
    return lax.dot_general(
        left,
        right,
        (((left_dim,), (right_dim,)), ((), ())),
        precision=HIGHEST,
        preferred_element_type=jnp.float32,
    )


def swap(array, axis, step):
    count = lax.axis_size(axis)
    return lax.ppermute(array, axis, [(i, i ^ step) for i in range(count)])


def scatter_sum(pieces, axis):
    total = pieces[0]
    for step in range(1, pieces.shape[0]):
        total = total + swap(pieces[step], axis, step)
    return total


def gather(piece, axis):
    count = lax.axis_size(axis)
    return jnp.stack([piece] + [swap(piece, axis, step) for step in range(1, count)])


def full_sum(piece, axis):
    count = lax.axis_size(axis)
    terms = [piece] + [swap(piece, axis, step) for step in range(1, count)]
    while len(terms) > 1:
        terms = [a + b for a, b in zip(terms[::2], terms[1::2])]
    return terms[0]


def prepared_kernel(where_ref, ends_ref, block_ref, out_ref):
    x, k, z, y = (where_ref[i] for i in range(4))
    step = pl.program_id(0)
    slab = (z ^ (step // 4)) * 4 + (y ^ (step % 4))
    slab_rows, width = block_ref.shape
    center = 0.5 * (ends_ref[0] + ends_ref[1])
    half_width = 0.5 * (ends_ref[1] - ends_ref[0])
    first_row = (2 * x + k) * (slab_rows * 16) + slab * slab_rows
    first_col = (4 * z + y) * width
    rows = lax.broadcasted_iota(jnp.int32, (slab_rows, 128), 0)
    lanes = lax.broadcasted_iota(jnp.int32, (slab_rows, 128), 1)
    low = lanes < 64
    blocks = []
    for s in range(4):
        at = pl.multiple_of((x ^ s) * 128, 128)
        values = block_ref[:, pl.ds(at, 128)]
        on = rows + first_row == lanes + (first_col + at)
        values = jnp.where(on, values - center, values) / half_width
        turned = pltpu.roll(values, 64, 1)
        blocks.append((jnp.where(k == 1, turned, values), jnp.where(k == 1, values, turned)))
    for j in range(2):
        (a, a_turned), (b, b_turned) = blocks[2 * j], blocks[2 * j + 1]
        out_ref[:, 128 * j : 128 * j + 128] = jnp.where(low, a, b_turned)
        out_ref[:, 256 + 128 * j : 384 + 128 * j] = jnp.where(low, a_turned, b)


def prepared(matrix, interval, where):
    rows, width = matrix.shape
    slab_rows = rows // 16
    z_y = lambda i, w: ((w[2] ^ (i // 4)) * 4 + (w[3] ^ (i % 4)), 0)
    return pl.pallas_call(
        prepared_kernel,
        grid_spec=pltpu.PrefetchScalarGridSpec(
            num_scalar_prefetch=2,
            grid=(16,),
            in_specs=[pl.BlockSpec((slab_rows, width), lambda i, w, e: z_y(i, w))],
            out_specs=pl.BlockSpec((slab_rows, width), lambda i, w, e: (i, 0)),
        ),
        out_shape=jax.ShapeDtypeStruct((rows, width), jnp.float32),
    )(where, interval, matrix)


def owner(slab):
    return (slab % 8) * 16 + slab // 8


def shards(matrix, start_vectors, interval):
    slab, width = start_vectors.shape
    half = width // 2
    total_rows = slab * 128
    x, k, z, y = (lax.axis_index(a) for a in ALL)
    row_index = 2 * x + k
    col_index = 4 * z + y
    operator = prepared(matrix, interval, jnp.stack([x, k, z, y]).astype(jnp.int32))

    def row_sum(partial, first, second):
        pieces = partial.reshape(4, 4, slab, half)
        if first == "y":
            pieces = pieces.transpose(1, 0, 2, 3)
        return scatter_sum(scatter_sum(pieces, first), second)

    def row_gather(piece, first, second):
        pieces = gather(gather(piece, second), first)
        if first == "y":
            pieces = pieces.transpose(1, 0, 2, 3)
        return pieces.reshape(16 * slab, half)

    def col_sum(partial):
        return scatter_sum(scatter_sum(partial.reshape(2, 4, slab, -1), "k"), "x")

    def col_gather(piece):
        return gather(gather(piece, "x"), "k").reshape(8 * slab, -1)

    def forward(cols):
        return [row_sum(dot(operator, v), *o) for v, o in zip(cols, orders)]

    def backward(rows):
        return [col_sum(dot(operator, v, 0, 0)) for v in rows]

    def gather_rows(slabs):
        return [row_gather(v, *o) for v, o in zip(slabs, orders)]

    def gather_cols(slabs):
        return [col_gather(v) for v in slabs]

    def twice_minus(new, old):
        return [2.0 * a - b for a, b in zip(new, old)]

    def join(halves):
        return jnp.concatenate(halves, axis=1)

    def split(array):
        return [array[:, :half], array[:, half:]]

    def columns_of(halves, index, count):
        size = width // count
        side = jnp.where(index < count // 2, halves[0], halves[1])
        return lax.dynamic_slice_in_dim(side, (index % (count // 2)) * size, size, 1)

    def in_row_order(pieces):
        parts = [
            lax.dynamic_slice(pieces, (k ^ (i % 2), x ^ (i // 2), 0, 0), (1, 1) + pieces.shape[2:])
            for i in range(8)
        ]
        return jnp.concatenate(parts).reshape(-1, pieces.shape[-1])

    def in_col_order(pieces):
        parts = [
            lax.dynamic_slice(pieces, (z ^ (i // 4), y ^ (i % 4), 0, 0), (1, 1) + pieces.shape[2:])
            for i in range(16)
        ]
        return jnp.concatenate(parts).reshape(-1, pieces.shape[-1])

    def inverse_factor(gram):
        factor = jnp.linalg.cholesky(gram)
        return jax.scipy.linalg.solve_triangular(factor, jnp.eye(width, dtype=jnp.float32), lower=True)

    orders = (("z", "y"), ("y", "z"))

    start = split(start_vectors)
    gathered = []
    start_slabs = []
    for value, (first, second) in zip(start, orders):
        pieces = []
        for step in range(4):
            turn = step if second == "y" else 4 * step
            moves = []
            for device in range(128):
                moves.append((owner(device ^ turn), device))
            pieces.append(lax.ppermute(value, ALL, moves))
        start_slabs.append(pieces[0])
        pieces = gather(jnp.stack(pieces), first)
        if first == "y":
            pieces = pieces.transpose(1, 0, 2, 3)
        gathered.append(pieces.reshape(16 * slab, half))

    first_slabs = backward(gathered)
    second_slabs = twice_minus(forward(gather_cols(first_slabs)), start_slabs)
    third_slabs = twice_minus(backward(gather_rows(second_slabs)), first_slabs)
    third_cols = gather_cols(third_slabs)

    gram_slice = dot(columns_of(third_cols, row_index, 8), join(third_cols), 0, 0)
    gram_slice = full_sum(full_sum(gram_slice, "y"), "z")
    gram = in_row_order(gather(gather(gram_slice, "x"), "k")) / total_rows
    inverse = inverse_factor(gram)

    first_slabs = forward(third_cols)
    second_slabs = twice_minus(backward(gather_rows(first_slabs)), third_slabs)
    third_slabs = twice_minus(forward(gather_cols(second_slabs)), first_slabs)
    third_slabs = split(dot(join(third_slabs), inverse, 1, 1))
    third_rows = gather_rows(third_slabs)
    back = [(device, owner(device)) for device in range(128)]
    final_slab = lax.ppermute(join(third_slabs), ALL, back)
    final_cols = col_gather(final_slab)

    gram_slice = dot(columns_of(third_rows, col_index, 16), join(third_rows), 0, 0)
    gram_slice = full_sum(full_sum(gram_slice, "k"), "x")
    gram = in_col_order(gather(gather(gram_slice, "y"), "z")) / total_rows
    inverse = inverse_factor(gram)

    mapped = join([dot(operator, v, 0, 0) for v in third_rows])
    cross = dot(final_cols, mapped, 0, 0).reshape(4, 2, -1, width)
    cross = jnp.concatenate(
        [lax.dynamic_slice(cross, (x ^ s, k ^ t, 0, 0), (1, 1) + cross.shape[2:]) for t in range(2) for s in range(4)]
    ).reshape(2, 4, -1, width)
    mapped_slab = col_sum(mapped)
    cross = scatter_sum(scatter_sum(cross, "k"), "x")
    cross = full_sum(full_sum(cross, "y"), "z")
    cross = in_row_order(gather(gather(cross, "x"), "k")) / total_rows

    projected = dot(dot(inverse, cross), inverse, 1, 1)
    basis = dot(final_slab, inverse, 1, 1)
    residual = dot(mapped_slab, inverse, 1, 1) - dot(basis, projected)
    return basis, projected, residual


def solution(mesh):
    torus = Mesh(mesh.devices.reshape(4, 2, 4, 4), ALL)
    placed = (P(ROW, COL), P(COL + ROW, None), P())
    return jax.shard_map(
        shards,
        mesh=torus,
        in_specs=placed,
        out_specs=(P(COL + ROW, None), P(), P(COL + ROW, None)),
        check_vma=False,
    )
```

```python
import functools

import jax
import jax.numpy as jnp
from jax import lax
from jax.experimental import pallas as pl
from jax.experimental.pallas import tpu as pltpu
from jax.sharding import Mesh
from jax.sharding import PartitionSpec as P


ALL = ("x", "k", "z", "y")
ROW = ("x", "k")
COL = ("z", "y")
HIGHEST = lax.Precision.HIGHEST


def dot(left, right, left_dim=1, right_dim=0):
    return lax.dot_general(
        left,
        right,
        (((left_dim,), (right_dim,)), ((), ())),
        precision=HIGHEST,
        preferred_element_type=jnp.float32,
    )


def swap(array, axis, step):
    count = lax.axis_size(axis)
    return lax.ppermute(array, axis, [(i, i ^ step) for i in range(count)])


def scatter_sum(pieces, axis):
    total = pieces[0]
    for step in range(1, pieces.shape[0]):
        total = total + swap(pieces[step], axis, step)
    return total


def gather(piece, axis):
    count = lax.axis_size(axis)
    return jnp.stack([piece] + [swap(piece, axis, step) for step in range(1, count)])


def full_sum(piece, axis):
    count = lax.axis_size(axis)
    terms = [piece] + [swap(piece, axis, step) for step in range(1, count)]
    while len(terms) > 1:
        terms = [a + b for a, b in zip(terms[::2], terms[1::2])]
    return terms[0]


def prepared_kernel(where_ref, ends_ref, block_ref, out_ref):
    x, k, z, y = (where_ref[i] for i in range(4))
    step = pl.program_id(0)
    slab = (z ^ (step // 4)) * 4 + (y ^ (step % 4))
    slab_rows, width = block_ref.shape
    center = 0.5 * (ends_ref[0] + ends_ref[1])
    half_width = 0.5 * (ends_ref[1] - ends_ref[0])
    first_row = (2 * x + k) * (slab_rows * 16) + slab * slab_rows
    first_col = (4 * z + y) * width
    rows = lax.broadcasted_iota(jnp.int32, (slab_rows, 128), 0)
    lanes = lax.broadcasted_iota(jnp.int32, (slab_rows, 128), 1)
    low = lanes < 64
    blocks = []
    for s in range(4):
        at = pl.multiple_of((x ^ s) * 128, 128)
        values = block_ref[:, pl.ds(at, 128)]
        on = rows + first_row == lanes + (first_col + at)
        values = jnp.where(on, values - center, values) / half_width
        turned = pltpu.roll(values, 64, 1)
        blocks.append((jnp.where(k == 1, turned, values), jnp.where(k == 1, values, turned)))
    for j in range(2):
        (a, a_turned), (b, b_turned) = blocks[2 * j], blocks[2 * j + 1]
        out_ref[:, 128 * j : 128 * j + 128] = jnp.where(low, a, b_turned)
        out_ref[:, 256 + 128 * j : 384 + 128 * j] = jnp.where(low, a_turned, b)


def prepared(matrix, interval, where):
    rows, width = matrix.shape
    slab_rows = rows // 16
    z_y = lambda i, w: ((w[2] ^ (i // 4)) * 4 + (w[3] ^ (i % 4)), 0)
    return pl.pallas_call(
        prepared_kernel,
        grid_spec=pltpu.PrefetchScalarGridSpec(
            num_scalar_prefetch=2,
            grid=(16,),
            in_specs=[pl.BlockSpec((slab_rows, width), lambda i, w, e: z_y(i, w))],
            out_specs=pl.BlockSpec((slab_rows, width), lambda i, w, e: (i, 0)),
        ),
        out_shape=jax.ShapeDtypeStruct((rows, width), jnp.float32),
    )(where, interval, matrix)


def panel(aug_ref, p):
    base = 16 * p
    rows = []
    for i in range(16):
        rows.append([
            jnp.broadcast_to(aug_ref[base + i : base + i + 1, :128], (8, 128)),
            jnp.broadcast_to(aug_ref[base + i : base + i + 1, 128:], (8, 128)),
        ])
    splat = {}
    for i in range(16):
        for j in range(i, 16):
            splat[i, j] = jnp.broadcast_to(rows[i][0][:, base + j : base + j + 1], (8, 128))
    for j in range(16):
        d = splat[j, j]
        inv = lax.rsqrt(d)
        inv = inv * (1.5 - (0.5 * d) * (inv * inv))
        u = {}
        for i in range(j + 1, 16):
            u[i] = splat[j, i] * inv
        for a in range(j + 1, 16):
            for b in range(a, 16):
                splat[a, b] = splat[a, b] - u[a] * u[b]
        for t in range(2):
            rows[j][t] = rows[j][t] * inv
        for i in range(j + 1, 16):
            for t in range(2):
                rows[i][t] = rows[i][t] - u[i] * rows[j][t]
    for i in range(16):
        for t in range(2):
            aug_ref[base + i : base + i + 1, 128 * t : 128 * t + 128] = rows[i][t][:1]


def factor_block(aug_ref):
    for p in range(8):
        panel(aug_ref, p)
        if p < 7:
            top = aug_ref[16 * p : 16 * p + 16, :]
            low = 16 * (p + 1)
            aug_ref[low:, :] = aug_ref[low:, :] - dot(top[:, :128], top, 0, 0)[low:, :]


def inverse_kernel(scale, place_ref, pieces_ref, out_ref, work_ref, aug_ref):
    count, size, n = pieces_ref.shape
    for i in range(count):
        at = pl.multiple_of(place_ref[i] * size, size)
        work_ref[pl.ds(at, size), :n] = pieces_ref[i] * scale
    rows = lax.broadcasted_iota(jnp.int32, (n, n), 0)
    lanes = lax.broadcasted_iota(jnp.int32, (n, n), 1)
    work_ref[:, n:] = jnp.where(rows == lanes, 1.0, 0.0)
    unit = jnp.where(rows[:128, :128] == lanes[:128, :128], 1.0, 0.0)

    def step(b, carry):
        at = pl.multiple_of(b * 128, 128)
        aug_ref[:, :128] = work_ref[pl.ds(at, 128), pl.ds(at, 128)]
        aug_ref[:, 128:] = unit
        factor_block(aug_ref)
        done = dot(aug_ref[:, 128:], work_ref[pl.ds(at, 128), :])
        out_ref[pl.ds(at, 128), :] = done[:, n:]
        later = jnp.where(lanes[:128] >= at + 128, done[:, :n], 0.0)
        work_ref[...] = work_ref[...] - dot(later, done, 0, 0)
        return carry

    lax.fori_loop(0, n // 128, step, 0)


def inverse_factor(pieces, place, scale):
    n = pieces.shape[-1]
    vmem = pl.BlockSpec(memory_space=pltpu.VMEM)
    return pl.pallas_call(
        functools.partial(inverse_kernel, scale),
        in_specs=[pl.BlockSpec(memory_space=pltpu.SMEM), vmem],
        out_specs=vmem,
        out_shape=jax.ShapeDtypeStruct((n, n), jnp.float32),
        scratch_shapes=[pltpu.VMEM((n, 2 * n), jnp.float32), pltpu.VMEM((128, 256), jnp.float32)],
        compiler_params=pltpu.CompilerParams(vmem_limit_bytes=24 * 2**20),
    )(place, pieces)


def owner(slab):
    return (slab % 8) * 16 + slab // 8


def shards(matrix, start_vectors, interval):
    slab, width = start_vectors.shape
    half = width // 2
    total_rows = slab * 128
    x, k, z, y = (lax.axis_index(a) for a in ALL)
    row_index = 2 * x + k
    col_index = 4 * z + y
    operator = prepared(matrix, interval, jnp.stack([x, k, z, y]).astype(jnp.int32))

    def row_sum(partial, first, second):
        pieces = partial.reshape(4, 4, slab, half)
        if first == "y":
            pieces = pieces.transpose(1, 0, 2, 3)
        return scatter_sum(scatter_sum(pieces, first), second)

    def row_gather(piece, first, second):
        pieces = gather(gather(piece, second), first)
        if first == "y":
            pieces = pieces.transpose(1, 0, 2, 3)
        return pieces.reshape(16 * slab, half)

    def col_sum(partial):
        return scatter_sum(scatter_sum(partial.reshape(2, 4, slab, -1), "k"), "x")

    def col_gather(piece):
        return gather(gather(piece, "x"), "k").reshape(8 * slab, -1)

    def forward(cols):
        return [row_sum(dot(operator, v), *o) for v, o in zip(cols, orders)]

    def backward(rows):
        return [col_sum(dot(operator, v, 0, 0)) for v in rows]

    def gather_rows(slabs):
        return [row_gather(v, *o) for v, o in zip(slabs, orders)]

    def gather_cols(slabs):
        return [col_gather(v) for v in slabs]

    def twice_minus(new, old):
        return [2.0 * a - b for a, b in zip(new, old)]

    def join(halves):
        return jnp.concatenate(halves, axis=1)

    def split(array):
        return [array[:, :half], array[:, half:]]

    def columns_of(halves, index, count):
        size = width // count
        side = jnp.where(index < count // 2, halves[0], halves[1])
        return lax.dynamic_slice_in_dim(side, (index % (count // 2)) * size, size, 1)

    def in_row_order(pieces):
        parts = [
            lax.dynamic_slice(pieces, (k ^ (i % 2), x ^ (i // 2), 0, 0), (1, 1) + pieces.shape[2:])
            for i in range(8)
        ]
        return jnp.concatenate(parts).reshape(-1, pieces.shape[-1])

    orders = (("z", "y"), ("y", "z"))
    row_places = jnp.stack([2 * (x ^ s) + (k ^ t) for t in range(2) for s in range(4)]).astype(jnp.int32)
    col_places = jnp.stack([4 * (z ^ s) + (y ^ t) for s in range(4) for t in range(4)]).astype(jnp.int32)

    start = split(start_vectors)
    gathered = []
    start_slabs = []
    for value, (first, second) in zip(start, orders):
        pieces = []
        for step in range(4):
            turn = step if second == "y" else 4 * step
            moves = []
            for device in range(128):
                moves.append((owner(device ^ turn), device))
            pieces.append(lax.ppermute(value, ALL, moves))
        start_slabs.append(pieces[0])
        pieces = gather(jnp.stack(pieces), first)
        if first == "y":
            pieces = pieces.transpose(1, 0, 2, 3)
        gathered.append(pieces.reshape(16 * slab, half))

    first_slabs = backward(gathered)
    second_slabs = twice_minus(forward(gather_cols(first_slabs)), start_slabs)
    third_slabs = twice_minus(backward(gather_rows(second_slabs)), first_slabs)
    third_cols = gather_cols(third_slabs)

    gram_slice = dot(columns_of(third_cols, row_index, 8), join(third_cols), 0, 0)
    gram_slice = full_sum(full_sum(gram_slice, "y"), "z")
    gram = gather(gather(gram_slice, "x"), "k").reshape(8, -1, width)
    inverse = inverse_factor(gram, row_places, 1.0 / total_rows)

    first_slabs = forward(third_cols)
    second_slabs = twice_minus(backward(gather_rows(first_slabs)), third_slabs)
    third_slabs = twice_minus(forward(gather_cols(second_slabs)), first_slabs)
    third_slabs = split(dot(join(third_slabs), inverse, 1, 1))
    third_rows = gather_rows(third_slabs)
    back = [(device, owner(device)) for device in range(128)]
    final_slab = lax.ppermute(join(third_slabs), ALL, back)
    final_cols = col_gather(final_slab)

    gram_slice = dot(columns_of(third_rows, col_index, 16), join(third_rows), 0, 0)
    gram_slice = full_sum(full_sum(gram_slice, "k"), "x")
    gram = gather(gather(gram_slice, "y"), "z").reshape(16, -1, width)
    inverse = inverse_factor(gram, col_places, 1.0 / total_rows)

    mapped = join([dot(operator, v, 0, 0) for v in third_rows])
    cross = dot(final_cols, mapped, 0, 0).reshape(4, 2, -1, width)
    cross = jnp.concatenate(
        [lax.dynamic_slice(cross, (x ^ s, k ^ t, 0, 0), (1, 1) + cross.shape[2:]) for t in range(2) for s in range(4)]
    ).reshape(2, 4, -1, width)
    mapped_slab = col_sum(mapped)
    cross = scatter_sum(scatter_sum(cross, "k"), "x")
    cross = full_sum(full_sum(cross, "y"), "z")
    cross = in_row_order(gather(gather(cross, "x"), "k")) / total_rows

    projected = dot(dot(inverse, cross), inverse, 1, 1)
    basis = dot(final_slab, inverse, 1, 1)
    residual = dot(mapped_slab, inverse, 1, 1) - dot(basis, projected)
    return basis, projected, residual


def solution(mesh):
    torus = Mesh(mesh.devices.reshape(4, 2, 4, 4), ALL)
    placed = (P(ROW, COL), P(COL + ROW, None), P())
    return jax.shard_map(
        shards,
        mesh=torus,
        in_specs=placed,
        out_specs=(P(COL + ROW, None), P(), P(COL + ROW, None)),
        check_vma=False,
    )
```

```python
import functools

import jax
import jax.numpy as jnp
from jax import lax
from jax.experimental import pallas as pl
from jax.experimental.pallas import tpu as pltpu
from jax.sharding import Mesh
from jax.sharding import PartitionSpec as P


ALL = ("x", "k", "z", "y")
CHIPS = ("x", "z", "y")
ROW = ("x", "k")
COL = ("z", "y")
HIGHEST = lax.Precision.HIGHEST


def dot(left, right, left_dim=1, right_dim=0):
    return lax.dot_general(
        left,
        right,
        (((left_dim,), (right_dim,)), ((), ())),
        precision=HIGHEST,
        preferred_element_type=jnp.float32,
    )


def swap(array, axis, step):
    count = lax.axis_size(axis)
    return lax.ppermute(array, axis, [(i, i ^ step) for i in range(count)])


def scatter_sum(pieces, axis):
    total = pieces[0]
    for step in range(1, pieces.shape[0]):
        total = total + swap(pieces[step], axis, step)
    return total


def gather(piece, axis):
    count = lax.axis_size(axis)
    return jnp.stack([piece] + [swap(piece, axis, step) for step in range(1, count)])


def full_sum(piece, axis):
    count = lax.axis_size(axis)
    terms = [piece] + [swap(piece, axis, step) for step in range(1, count)]
    while len(terms) > 1:
        terms = [a + b for a, b in zip(terms[::2], terms[1::2])]
    return terms[0]


def slab_at(step, where, half, inner):
    outer, inner = step // 2, 2 * (step % 2) + inner
    along_z, along_y = (outer, inner) if half == 0 else (inner, outer)
    return 4 * (where[2] ^ along_z) + (where[3] ^ along_y)


def prepared_kernel(half, where_ref, ends_ref, *refs):
    *piece_refs, out_ref, turned_ref = refs
    x, k, z, y = (where_ref[i] for i in range(4))
    size, width = piece_refs[0].shape
    center = 0.5 * (ends_ref[0] + ends_ref[1])
    half_width = 0.5 * (ends_ref[1] - ends_ref[0])
    first_col = (4 * z + y) * width
    rows = lax.broadcasted_iota(jnp.int32, (size, 128), 0)
    lanes = lax.broadcasted_iota(jnp.int32, (size, 128), 1)
    for inner in range(2):
        slab = slab_at(pl.program_id(0), where_ref, half, inner)
        first_row = x * (32 * size) + slab * (2 * size) + half * size
        mine = slab // 8 == k
        for s in range(4):
            at = pl.multiple_of((x ^ s) * 128, 128)
            own = piece_refs[2 * inner][:, pl.ds(at, 128)]
            other = piece_refs[2 * inner + 1][:, pl.ds(at, 128)]
            values = jnp.where(mine, own, other)
            on = rows + first_row == lanes + (first_col + at)
            values = jnp.where(on, values - center, values) / half_width
            out_ref[size * inner : size * (inner + 1), 128 * s : 128 * (s + 1)] = values
    for s in range(4):
        turned_ref[128 * s : 128 * (s + 1), :] = out_ref[:, 128 * s : 128 * (s + 1)].T


def prepared(own, other, interval, where, half):
    rows, width = own.shape
    size = rows // 16
    pieces = [
        pl.BlockSpec((size, width), lambda i, w, e, n=n: ((2 * slab_at(i, w, half, n) + half) % 16, 0))
        for n in range(2)
    ]
    return pl.pallas_call(
        functools.partial(prepared_kernel, half),
        grid_spec=pltpu.PrefetchScalarGridSpec(
            num_scalar_prefetch=2,
            grid=(8,),
            in_specs=[pieces[0], pieces[0], pieces[1], pieces[1]],
            out_specs=[
                pl.BlockSpec((2 * size, width), lambda i, w, e: (i, 0)),
                pl.BlockSpec((width, 2 * size), lambda i, w, e: (0, i)),
            ],
        ),
        out_shape=[
            jax.ShapeDtypeStruct((rows, width), jnp.float32),
            jax.ShapeDtypeStruct((width, rows), jnp.float32),
        ],
    )(where, interval, own, other, own, other)


def panel(aug_ref, p):
    base = 16 * p
    rows = []
    for i in range(16):
        rows.append([
            jnp.broadcast_to(aug_ref[base + i : base + i + 1, :128], (8, 128)),
            jnp.broadcast_to(aug_ref[base + i : base + i + 1, 128:], (8, 128)),
        ])
    splat = {}
    for i in range(16):
        for j in range(i, 16):
            splat[i, j] = jnp.broadcast_to(rows[i][0][:, base + j : base + j + 1], (8, 128))
    for j in range(16):
        d = splat[j, j]
        inv = lax.rsqrt(d)
        inv = inv * (1.5 - (0.5 * d) * (inv * inv))
        u = {}
        for i in range(j + 1, 16):
            u[i] = splat[j, i] * inv
        for a in range(j + 1, 16):
            for b in range(a, 16):
                splat[a, b] = splat[a, b] - u[a] * u[b]
        for t in range(2):
            rows[j][t] = rows[j][t] * inv
        for i in range(j + 1, 16):
            for t in range(2):
                rows[i][t] = rows[i][t] - u[i] * rows[j][t]
    for i in range(16):
        for t in range(2):
            aug_ref[base + i : base + i + 1, 128 * t : 128 * t + 128] = rows[i][t][:1]


def factor_block(aug_ref):
    for p in range(8):
        panel(aug_ref, p)
        if p < 7:
            top = aug_ref[16 * p : 16 * p + 16, :]
            low = 16 * (p + 1)
            aug_ref[low:, :] = aug_ref[low:, :] - dot(top[:, :128], top, 0, 0)[low:, :]


def inverse_kernel(scale, place_ref, pieces_ref, out_ref, work_ref, aug_ref):
    count, size, n = pieces_ref.shape
    for i in range(count):
        at = pl.multiple_of(place_ref[i] * size, size)
        work_ref[pl.ds(at, size), :n] = pieces_ref[i] * scale
    rows = lax.broadcasted_iota(jnp.int32, (n, n), 0)
    lanes = lax.broadcasted_iota(jnp.int32, (n, n), 1)
    work_ref[:, n:] = jnp.where(rows == lanes, 1.0, 0.0)
    unit = jnp.where(rows[:128, :128] == lanes[:128, :128], 1.0, 0.0)

    def step(b, carry):
        at = pl.multiple_of(b * 128, 128)
        aug_ref[:, :128] = work_ref[pl.ds(at, 128), pl.ds(at, 128)]
        aug_ref[:, 128:] = unit
        factor_block(aug_ref)
        done = dot(aug_ref[:, 128:], work_ref[pl.ds(at, 128), :])
        out_ref[pl.ds(at, 128), :] = done[:, n:]
        later = jnp.where(lanes[:128] >= at + 128, done[:, :n], 0.0)
        work_ref[...] = work_ref[...] - dot(later, done, 0, 0)
        return carry

    lax.fori_loop(0, n // 128, step, 0)


def inverse_factor(pieces, place, scale):
    n = pieces.shape[-1]
    vmem = pl.BlockSpec(memory_space=pltpu.VMEM)
    return pl.pallas_call(
        functools.partial(inverse_kernel, scale),
        in_specs=[pl.BlockSpec(memory_space=pltpu.SMEM), vmem],
        out_specs=vmem,
        out_shape=jax.ShapeDtypeStruct((n, n), jnp.float32),
        scratch_shapes=[pltpu.VMEM((n, 2 * n), jnp.float32), pltpu.VMEM((128, 256), jnp.float32)],
        compiler_params=pltpu.CompilerParams(vmem_limit_bytes=24 * 2**20),
    )(place, pieces)


def owner(slab):
    return (slab % 4) * 16 + slab // 4


def shards(matrix, start_vectors, interval):
    slab, width = start_vectors.shape
    half = width // 2
    total_rows = slab * 128
    x, k, z, y = (lax.axis_index(a) for a in ALL)
    south = k == 0
    where = jnp.stack([x, k, z, y]).astype(jnp.int32)
    row_places = jnp.stack([2 * (x ^ s) + (k ^ t) for t in range(2) for s in range(4)]).astype(jnp.int32)
    col_places = jnp.stack([4 * (z ^ s) + (y ^ t) for s in range(4) for t in range(4)]).astype(jnp.int32)

    orders = (("z", "y"), ("y", "z"))

    def gather_rows(slabs):
        return [gather(gather(v, b), a).reshape(16 * slab, half) for v, (a, b) in zip(slabs, orders)]

    def gather_cols(pair):
        return gather(pair, "x").reshape(8 * slab, half)

    def forward(cols):
        out = []
        for (plain, turned), (a, b) in zip(operator, orders):
            partial = dot(plain, cols).reshape(4, 4, slab, half)
            out.append(scatter_sum(scatter_sum(partial, a), b))
        return out

    def mapped_part(rows):
        (_, first), (_, second) = operator
        return dot(first, rows[0]) + dot(second, rows[1])

    def col_sum(partial):
        return scatter_sum(partial.reshape(4, 2 * slab, half), "x")

    def twice_minus(new, old):
        return jax.tree.map(lambda a, b: 2.0 * a - b, new, old)

    def in_order(mine, other, axis=1):
        return jnp.concatenate([jnp.where(south, mine, other), jnp.where(south, other, mine)], axis=axis)

    def of_half(array, index, axis):
        size = array.shape[axis] // 2
        return lax.dynamic_slice_in_dim(array, index * size, size, axis)

    def gram_slice(mine, other, index, count):
        size = width // count
        side = jnp.where(index // (count // 2) == k, mine, other)
        side = lax.dynamic_slice_in_dim(side, (index % (count // 2)) * size, size, 1)
        return in_order(dot(side, mine, 0, 0), dot(side, other, 0, 0))

    def by_x(pieces):
        return jnp.concatenate([lax.dynamic_slice_in_dim(pieces, x ^ s, 1, 0) for s in range(4)])

    received = swap(of_half(start_vectors, 1 - k, 1), "k", 1)
    kept = of_half(start_vectors, k, 1)
    pairs = (jnp.where(south, kept, received), jnp.where(south, received, kept))
    start_slabs = []
    start_rows = []
    for value, (first, second) in zip(pairs, orders):
        pieces = []
        for step in range(4):
            turn = step if second == "y" else 4 * step
            moves = [(owner(chip ^ turn), chip) for chip in range(64)]
            pieces.append(lax.ppermute(value, CHIPS, moves))
        start_slabs.append(pieces[0])
        start_rows.append(gather(jnp.stack(pieces), first).reshape(16 * slab, half))

    other_matrix = swap(matrix, "k", 1)
    operator = [prepared(matrix, other_matrix, interval, where, h) for h in range(2)]

    first = col_sum(mapped_part(start_rows))
    second = twice_minus(forward(gather_cols(first)), start_slabs)
    third = twice_minus(col_sum(mapped_part(gather_rows(second))), first)
    third_cols = gather_cols(third)

    part = gram_slice(third_cols, swap(third_cols, "k", 1), 2 * x + k, 8)
    part = full_sum(full_sum(part, "y"), "z")
    gram = gather(gather(part, "x"), "k").reshape(8, -1, width)
    inverse = inverse_factor(gram, row_places, 1.0 / total_rows)

    first = forward(third_cols)
    second = twice_minus(col_sum(mapped_part(gather_rows(first))), third)
    third = jnp.concatenate(twice_minus(forward(gather_cols(second)), first))
    third = in_order(third, swap(third, "k", 1))
    third = dot(third, of_half(inverse, k, 0), 1, 1)
    third_rows = gather_rows([third[:slab], third[slab:]])

    final = lax.ppermute(third, CHIPS, [(chip, owner(chip)) for chip in range(64)])
    final_cols = gather_cols(final)
    final_cols = in_order(final_cols, swap(final_cols, "k", 1))
    final_slab = lax.dynamic_slice_in_dim(final_cols, k * slab, slab, 0)

    mine = jnp.where(south, third_rows[0], third_rows[1])
    other = swap(jnp.where(south, third_rows[1], third_rows[0]), "k", 1)
    part = gram_slice(mine, other, 4 * z + y, 16)
    part = full_sum(full_sum(part, "k"), "x")
    gram = gather(gather(part, "y"), "z").reshape(16, -1, width)
    inverse = inverse_factor(gram, col_places, 1.0 / total_rows)

    mapped = mapped_part(third_rows)
    cross = by_x(dot(final_cols, mapped, 0, 0).reshape(4, -1, half))
    cross = scatter_sum(cross, "x")
    cross = full_sum(full_sum(cross, "y"), "z")
    cross = by_x(gather(cross, "x")).reshape(width, half)
    cross = in_order(cross, swap(cross, "k", 1)) / total_rows

    mapped = col_sum(mapped)
    mapped_slab = in_order(of_half(mapped, k, 0), swap(of_half(mapped, 1 - k, 0), "k", 1))

    projected = dot(dot(inverse, cross), inverse, 1, 1)
    basis = dot(final_slab, inverse, 1, 1)
    residual = dot(mapped_slab, inverse, 1, 1) - dot(basis, projected)
    return basis, projected, residual


def solution(mesh):
    torus = Mesh(mesh.devices.reshape(4, 2, 4, 4), ALL)
    placed = (P(ROW, COL), P(COL + ROW, None), P())
    return jax.shard_map(
        shards,
        mesh=torus,
        in_specs=placed,
        out_specs=(P(COL + ROW, None), P(), P(COL + ROW, None)),
        check_vma=False,
    )
```

```python
import functools

import jax
import jax.numpy as jnp
from jax import lax
from jax.experimental import pallas as pl
from jax.experimental.pallas import tpu as pltpu
from jax.sharding import Mesh
from jax.sharding import PartitionSpec as P


ALL = ("x", "k", "z", "y")
CHIPS = ("x", "z", "y")
ROW = ("x", "k")
COL = ("z", "y")
HIGHEST = lax.Precision.HIGHEST


def dot(left, right, left_dim=1, right_dim=0):
    return lax.dot_general(
        left,
        right,
        (((left_dim,), (right_dim,)), ((), ())),
        precision=HIGHEST,
        preferred_element_type=jnp.float32,
    )


def swap(array, axis, step):
    count = lax.axis_size(axis)
    return lax.ppermute(array, axis, [(i, i ^ step) for i in range(count)])


def scatter_sum(pieces, axis):
    total = pieces[0]
    for step in range(1, pieces.shape[0]):
        total = total + swap(pieces[step], axis, step)
    return total


def gather(piece, axis):
    count = lax.axis_size(axis)
    return jnp.stack([piece] + [swap(piece, axis, step) for step in range(1, count)])


def full_sum(piece, axis, along=False):
    count = lax.axis_size(axis)
    terms = [piece]
    for step in range(1, count):
        term = swap(piece, axis, step)
        if along:
            term = term.reshape(2, 2, *piece.shape[1:])
            term = jnp.flip(term, [d for d in range(2) if step & (2 >> d)]).reshape(piece.shape)
        terms.append(term)
    while len(terms) > 1:
        terms = [a + b for a, b in zip(terms[::2], terms[1::2])]
    return terms[0]


def slab_at(step, where, half, inner):
    outer, inner = step // 2, 2 * (step % 2) + inner
    along_z, along_y = (outer, inner) if half == 0 else (inner, outer)
    return 4 * (where[2] ^ along_z) + (where[3] ^ along_y)


def prepared_kernel(half, where_ref, ends_ref, *refs):
    *piece_refs, out_ref, turned_ref = refs
    x, k, z, y = (where_ref[i] for i in range(4))
    size, width = piece_refs[0].shape
    center = 0.5 * (ends_ref[0] + ends_ref[1])
    half_width = 0.5 * (ends_ref[1] - ends_ref[0])
    first_col = (4 * z + y) * width
    rows = lax.broadcasted_iota(jnp.int32, (size, 128), 0)
    lanes = lax.broadcasted_iota(jnp.int32, (size, 128), 1)
    for inner in range(2):
        slab = slab_at(pl.program_id(0), where_ref, half, inner)
        first_row = x * (32 * size) + slab * (2 * size) + half * size
        mine = slab // 8 == k
        for s in range(4):
            at = pl.multiple_of((x ^ s) * 128, 128)
            own = piece_refs[2 * inner][:, pl.ds(at, 128)]
            other = piece_refs[2 * inner + 1][:, pl.ds(at, 128)]
            values = jnp.where(mine, own, other)
            on = rows + first_row == lanes + (first_col + at)
            values = jnp.where(on, values - center, values) / half_width
            out_ref[size * inner : size * (inner + 1), 128 * s : 128 * (s + 1)] = values
    for s in range(4):
        turned_ref[128 * s : 128 * (s + 1), :] = out_ref[:, 128 * s : 128 * (s + 1)].T


def prepared(own, other, interval, where, half):
    rows, width = own.shape
    size = rows // 16
    pieces = [
        pl.BlockSpec((size, width), lambda i, w, e, n=n: ((2 * slab_at(i, w, half, n) + half) % 16, 0))
        for n in range(2)
    ]
    return pl.pallas_call(
        functools.partial(prepared_kernel, half),
        grid_spec=pltpu.PrefetchScalarGridSpec(
            num_scalar_prefetch=2,
            grid=(8,),
            in_specs=[pieces[0], pieces[0], pieces[1], pieces[1]],
            out_specs=[
                pl.BlockSpec((2 * size, width), lambda i, w, e: (i, 0)),
                pl.BlockSpec((width, 2 * size), lambda i, w, e: (0, i)),
            ],
        ),
        out_shape=[
            jax.ShapeDtypeStruct((rows, width), jnp.float32),
            jax.ShapeDtypeStruct((width, rows), jnp.float32),
        ],
    )(where, interval, own, other, own, other)


def panel(aug_ref, p):
    base = 16 * p
    rows = []
    for i in range(16):
        rows.append([
            jnp.broadcast_to(aug_ref[base + i : base + i + 1, :128], (8, 128)),
            jnp.broadcast_to(aug_ref[base + i : base + i + 1, 128:], (8, 128)),
        ])
    splat = {}
    for i in range(16):
        for j in range(i, 16):
            splat[i, j] = jnp.broadcast_to(rows[i][0][:, base + j : base + j + 1], (8, 128))
    for j in range(16):
        d = splat[j, j]
        inv = lax.rsqrt(d)
        inv = inv * (1.5 - (0.5 * d) * (inv * inv))
        u = {}
        for i in range(j + 1, 16):
            u[i] = splat[j, i] * inv
        for a in range(j + 1, 16):
            for b in range(a, 16):
                splat[a, b] = splat[a, b] - u[a] * u[b]
        for t in range(2):
            rows[j][t] = rows[j][t] * inv
        for i in range(j + 1, 16):
            for t in range(2):
                rows[i][t] = rows[i][t] - u[i] * rows[j][t]
    for i in range(16):
        for t in range(2):
            aug_ref[base + i : base + i + 1, 128 * t : 128 * t + 128] = rows[i][t][:1]


def factor_block(aug_ref):
    for p in range(8):
        panel(aug_ref, p)
        if p < 7:
            top = aug_ref[16 * p : 16 * p + 16, :]
            low = 16 * (p + 1)
            aug_ref[low:, :] = aug_ref[low:, :] - dot(top[:, :128], top, 0, 0)[low:, :]


def inverse_kernel(scale, place_ref, pieces_ref, out_ref, work_ref, aug_ref):
    count, size, n = pieces_ref.shape
    for i in range(count):
        at = pl.multiple_of(place_ref[i] * size, size)
        work_ref[pl.ds(at, size), :n] = pieces_ref[i] * scale
    rows = lax.broadcasted_iota(jnp.int32, (n, n), 0)
    lanes = lax.broadcasted_iota(jnp.int32, (n, n), 1)
    work_ref[:, n:] = jnp.where(rows == lanes, 1.0, 0.0)
    unit = jnp.where(rows[:128, :128] == lanes[:128, :128], 1.0, 0.0)

    def step(b, carry):
        at = pl.multiple_of(b * 128, 128)
        aug_ref[:, :128] = work_ref[pl.ds(at, 128), pl.ds(at, 128)]
        aug_ref[:, 128:] = unit
        factor_block(aug_ref)
        done = dot(aug_ref[:, 128:], work_ref[pl.ds(at, 128), :])
        out_ref[pl.ds(at, 128), :] = done[:, n:]
        later = jnp.where(lanes[:128] >= at + 128, done[:, :n], 0.0)
        work_ref[...] = work_ref[...] - dot(later, done, 0, 0)
        return carry

    lax.fori_loop(0, n // 128, step, 0)


def inverse_factor(pieces, place, scale):
    n = pieces.shape[-1]
    vmem = pl.BlockSpec(memory_space=pltpu.VMEM)
    return pl.pallas_call(
        functools.partial(inverse_kernel, scale),
        in_specs=[pl.BlockSpec(memory_space=pltpu.SMEM), vmem],
        out_specs=vmem,
        out_shape=jax.ShapeDtypeStruct((n, n), jnp.float32),
        scratch_shapes=[pltpu.VMEM((n, 2 * n), jnp.float32), pltpu.VMEM((128, 256), jnp.float32)],
        compiler_params=pltpu.CompilerParams(vmem_limit_bytes=24 * 2**20),
    )(place, pieces)


def owner(slab):
    return (slab % 4) * 16 + slab // 4


def shards(matrix, start_vectors, interval):
    slab, width = start_vectors.shape
    half = width // 2
    total_rows = slab * 128
    x, k, z, y = (lax.axis_index(a) for a in ALL)
    south = k == 0
    where = jnp.stack([x, k, z, y]).astype(jnp.int32)
    places = jnp.stack([x ^ s for s in range(4)]).astype(jnp.int32)

    orders = (("z", "y"), ("y", "z"))

    def gather_rows(fours):
        return [gather(v, a).reshape(16 * slab, half) for v, (a, b) in zip(fours, orders)]

    def gather_cols(pair):
        return gather(pair, "x").reshape(8 * slab, half)

    def forward(cols):
        out = []
        for (plain, turned), (a, b) in zip(operator, orders):
            partial = dot(plain, cols).reshape(4, 4, slab, half)
            out.append(full_sum(scatter_sum(partial, a), b, along=True))
        return out

    def mapped_part(rows):
        (_, first), (_, second) = operator
        return dot(first, rows[0]) + dot(second, rows[1])

    def col_sum(partial):
        return scatter_sum(partial.reshape(4, 2 * slab, half), "x")

    def twice_minus(new, old):
        return jax.tree.map(lambda a, b: 2.0 * a - b, new, old)

    def in_order(mine, other, axis):
        return jnp.concatenate([jnp.where(south, mine, other), jnp.where(south, other, mine)], axis=axis)

    def of_half(array, index, axis):
        size = array.shape[axis] // 2
        return lax.dynamic_slice_in_dim(array, index * size, size, axis)

    def gram_part(mine, other):
        size = width // 4
        side = jnp.where(x // 2 == k, mine, other)
        side = lax.dynamic_slice_in_dim(side, (x % 2) * size, size, 1)
        return dot(side, mine, 0, 0)

    def by_x(pieces):
        return jnp.concatenate([lax.dynamic_slice_in_dim(pieces, x ^ s, 1, 0) for s in range(4)])

    received = swap(of_half(start_vectors, 1 - k, 1), "k", 1)
    kept = of_half(start_vectors, k, 1)
    pair = in_order(kept, received, 0)
    pair = lax.ppermute(pair, CHIPS, [(owner(chip), chip) for chip in range(64)])
    start = [gather(v, b) for v, (a, b) in zip((pair[:slab], pair[slab:]), orders)]

    other_matrix = swap(matrix, "k", 1)
    operator = [prepared(matrix, other_matrix, interval, where, h) for h in range(2)]

    first = col_sum(mapped_part(gather_rows(start)))
    second = twice_minus(forward(gather_cols(first)), start)
    third = twice_minus(col_sum(mapped_part(gather_rows(second))), first)
    third_cols = gather_cols(third)

    part = gram_part(third_cols, swap(third_cols, "k", 1))
    gram = gather(full_sum(full_sum(part, "y"), "z"), "x")
    gram = in_order(gram, swap(gram, "k", 1), 2)
    inverse = inverse_factor(gram, places, 1.0 / total_rows)

    first = forward(third_cols)
    second = twice_minus(col_sum(mapped_part(gather_rows(first))), third)
    third = jnp.concatenate(twice_minus(forward(gather_cols(second)), first)).reshape(8 * slab, half)
    third = in_order(third, swap(third, "k", 1), 1)
    third = dot(third, of_half(inverse, k, 0), 1, 1).reshape(2, 4, slab, half)
    third_rows = gather_rows(third)

    final = lax.ppermute(third[:, 0].reshape(2 * slab, half), CHIPS, [(chip, owner(chip)) for chip in range(64)])
    final_cols = gather_cols(final)
    other_cols = swap(final_cols, "k", 1)
    both_cols = in_order(final_cols, other_cols, 1)
    final_slab = lax.dynamic_slice_in_dim(both_cols, k * slab, slab, 0)

    mapped = mapped_part(third_rows)
    cross = by_x(dot(both_cols, mapped, 0, 0).reshape(4, -1, half))
    mapped, cross = scatter_sum(jnp.stack([mapped.reshape(cross.shape), cross], 1), "x")
    part = jnp.stack([gram_part(final_cols, other_cols), cross])
    part = gather(full_sum(full_sum(part, "y"), "z"), "x")
    part = in_order(part, swap(part, "k", 1), 3)
    inverse = inverse_factor(part[:, 0], places, 1.0 / total_rows)
    cross = by_x(part[:, 1]).reshape(width, width) / total_rows

    mapped_slab = in_order(of_half(mapped, k, 0), swap(of_half(mapped, 1 - k, 0), "k", 1), 1)
    projected = dot(dot(inverse, cross), inverse, 1, 1)
    basis = dot(final_slab, inverse, 1, 1)
    residual = dot(mapped_slab, inverse, 1, 1) - dot(basis, projected)
    return basis, projected, residual


def solution(mesh):
    torus = Mesh(mesh.devices.reshape(4, 2, 4, 4), ALL)
    placed = (P(ROW, COL), P(COL + ROW, None), P())
    return jax.shard_map(
        shards,
        mesh=torus,
        in_specs=placed,
        out_specs=(P(COL + ROW, None), P(), P(COL + ROW, None)),
        check_vma=False,
    )
```

```python
import functools

import jax
import jax.numpy as jnp
from jax import lax
from jax.experimental import pallas as pl
from jax.experimental.pallas import tpu as pltpu
from jax.sharding import Mesh
from jax.sharding import PartitionSpec as P


ALL = ("x", "k", "z", "y")
CHIPS = ("x", "z", "y")
ROW = ("x", "k")
COL = ("z", "y")
HIGHEST = lax.Precision.HIGHEST
HIGH = lax.Precision.HIGH


def dot(left, right, left_dim=1, right_dim=0, precision=HIGHEST):
    return lax.dot_general(
        left,
        right,
        (((left_dim,), (right_dim,)), ((), ())),
        precision=precision,
        preferred_element_type=jnp.float32,
    )


def swap(array, axis, step):
    count = lax.axis_size(axis)
    return lax.ppermute(array, axis, [(i, i ^ step) for i in range(count)])


def scatter_sum(pieces, axis):
    total = pieces[0]
    for step in range(1, pieces.shape[0]):
        total = total + swap(pieces[step], axis, step)
    return total


def gather(piece, axis):
    count = lax.axis_size(axis)
    return jnp.stack([piece] + [swap(piece, axis, step) for step in range(1, count)])


def full_sum(piece, axis, along=False):
    count = lax.axis_size(axis)
    terms = [piece]
    for step in range(1, count):
        term = swap(piece, axis, step)
        if along:
            term = term.reshape(2, 2, *piece.shape[1:])
            term = jnp.flip(term, [d for d in range(2) if step & (2 >> d)]).reshape(piece.shape)
        terms.append(term)
    while len(terms) > 1:
        terms = [a + b for a, b in zip(terms[::2], terms[1::2])]
    return terms[0]


def slab_at(step, where, half, inner):
    outer, inner = step // 2, 2 * (step % 2) + inner
    along_z, along_y = (outer, inner) if half == 0 else (inner, outer)
    return (where[2] ^ along_z) + 4 * (where[3] ^ along_y)


def prepared_kernel(half, where_ref, ends_ref, *refs):
    *piece_refs, out_ref, turned_ref = refs
    x, k, z, y = (where_ref[i] for i in range(4))
    size, width = piece_refs[0].shape
    center = 0.5 * (ends_ref[0] + ends_ref[1])
    half_width = 0.5 * (ends_ref[1] - ends_ref[0])
    first_col = (4 * z + y) * width
    rows = lax.broadcasted_iota(jnp.int32, (size, 128), 0)
    lanes = lax.broadcasted_iota(jnp.int32, (size, 128), 1)
    for inner in range(2):
        slab = slab_at(pl.program_id(0), where_ref, half, inner)
        first_row = x * (32 * size) + slab * (2 * size) + half * size
        mine = slab // 8 == k
        for s in range(4):
            at = pl.multiple_of((x ^ s) * 128, 128)
            own = piece_refs[2 * inner][:, pl.ds(at, 128)]
            other = piece_refs[2 * inner + 1][:, pl.ds(at, 128)]
            values = jnp.where(mine, own, other)
            on = rows + first_row == lanes + (first_col + at)
            values = jnp.where(on, values - center, values) / half_width
            out_ref[size * inner : size * (inner + 1), 128 * s : 128 * (s + 1)] = values
    for s in range(4):
        turned_ref[128 * s : 128 * (s + 1), :] = out_ref[:, 128 * s : 128 * (s + 1)].T


def prepared(own, other, interval, where, half):
    rows, width = own.shape
    size = rows // 16
    pieces = [
        pl.BlockSpec((size, width), lambda i, w, e, n=n: ((2 * slab_at(i, w, half, n) + half) % 16, 0))
        for n in range(2)
    ]
    return pl.pallas_call(
        functools.partial(prepared_kernel, half),
        grid_spec=pltpu.PrefetchScalarGridSpec(
            num_scalar_prefetch=2,
            grid=(8,),
            in_specs=[pieces[0], pieces[0], pieces[1], pieces[1]],
            out_specs=[
                pl.BlockSpec((2 * size, width), lambda i, w, e: (i, 0)),
                pl.BlockSpec((width, 2 * size), lambda i, w, e: (0, i)),
            ],
        ),
        out_shape=[
            jax.ShapeDtypeStruct((rows, width), jnp.float32),
            jax.ShapeDtypeStruct((width, rows), jnp.float32),
        ],
        cost_estimate=pl.CostEstimate(flops=10**9, transcendentals=0, bytes_accessed=16 * rows * width),
    )(where, interval, own, other, own, other)


def panel(aug_ref, p):
    base = 16 * p
    rows = []
    for i in range(16):
        rows.append([
            jnp.broadcast_to(aug_ref[base + i : base + i + 1, :128], (8, 128)),
            jnp.broadcast_to(aug_ref[base + i : base + i + 1, 128:], (8, 128)),
        ])
    splat = {}
    for i in range(16):
        for j in range(i, 16):
            splat[i, j] = jnp.broadcast_to(rows[i][0][:, base + j : base + j + 1], (8, 128))
    for j in range(16):
        inv = lax.rsqrt(splat[j, j])
        u = {}
        for i in range(j + 1, 16):
            u[i] = splat[j, i] * inv
        for a in range(j + 1, 16):
            for b in range(a, 16):
                splat[a, b] = splat[a, b] - u[a] * u[b]
        for t in range(2):
            rows[j][t] = rows[j][t] * inv
        for i in range(j + 1, 16):
            for t in range(2):
                rows[i][t] = rows[i][t] - u[i] * rows[j][t]
    for i in range(16):
        for t in range(2):
            aug_ref[base + i : base + i + 1, 128 * t : 128 * t + 128] = rows[i][t][:1]


def factor_block(aug_ref):
    for p in range(8):
        panel(aug_ref, p)
        if p < 7:
            low = 16 * (p + 1)
            above = aug_ref[:low, :]
            rows = aug_ref[low : low + 16, :]
            aug_ref[low : low + 16, :] = rows - dot(above[:, low : low + 16], above, 0, 0)


def inverse_kernel(scale, place_ref, pieces_ref, out_ref, work_ref, aug_ref):
    count, size, n = pieces_ref.shape
    for i in range(count):
        at = pl.multiple_of(place_ref[i] * size, size)
        work_ref[pl.ds(at, size), :n] = pieces_ref[i] * scale
    rows = lax.broadcasted_iota(jnp.int32, (n, n), 0)
    lanes = lax.broadcasted_iota(jnp.int32, (n, n), 1)
    work_ref[:, n:] = jnp.where(rows == lanes, 1.0, 0.0)
    unit = jnp.where(rows[:128, :128] == lanes[:128, :128], 1.0, 0.0)

    def step(b, carry):
        at = pl.multiple_of(b * 128, 128)
        aug_ref[:, :128] = work_ref[pl.ds(at, 128), pl.ds(at, 128)]
        aug_ref[:, 128:] = unit
        factor_block(aug_ref)
        done = dot(aug_ref[:, 128:], work_ref[pl.ds(at, 128), :])
        out_ref[pl.ds(at, 128), :] = done[:, n:]
        later = jnp.where(lanes[:128] >= at + 128, done[:, :n], 0.0)
        work_ref[...] = work_ref[...] - dot(later, done, 0, 0)
        return carry

    lax.fori_loop(0, n // 128, step, 0)


def inverse_factor(pieces, place, scale):
    n = pieces.shape[-1]
    vmem = pl.BlockSpec(memory_space=pltpu.VMEM)
    return pl.pallas_call(
        functools.partial(inverse_kernel, scale),
        in_specs=[pl.BlockSpec(memory_space=pltpu.SMEM), vmem],
        out_specs=vmem,
        out_shape=jax.ShapeDtypeStruct((n, n), jnp.float32),
        scratch_shapes=[pltpu.VMEM((n, 2 * n), jnp.float32), pltpu.VMEM((128, 256), jnp.float32)],
        compiler_params=pltpu.CompilerParams(vmem_limit_bytes=24 * 2**20),
        cost_estimate=pl.CostEstimate(flops=6 * 10**9, transcendentals=n, bytes_accessed=8 * n * n),
    )(place, pieces)


def turned(chip):
    return (chip // 4 % 4) * 16 + (chip // 16) * 4 + chip % 4


TURN = [(chip, turned(chip)) for chip in range(64)]


def shards(matrix, start_vectors, interval):
    slab, width = start_vectors.shape
    half = width // 2
    total_rows = slab * 128
    x, k, z, y = (lax.axis_index(a) for a in ALL)
    south = k == 0
    where = jnp.stack([x, k, z, y]).astype(jnp.int32)
    places = jnp.stack([x ^ s for s in range(4)]).astype(jnp.int32)

    orders = (("z", "y"), ("y", "z"))

    def gather_rows(fours):
        return [gather(v, a).reshape(16 * slab, half) for v, (a, b) in zip(fours, orders)]

    def gather_cols(pair):
        return gather(pair, "x").reshape(8 * slab, half)

    def forward(cols):
        out = []
        for (plain, across), (a, b) in zip(operator, orders):
            partial = dot(plain, cols, precision=HIGH).reshape(4, 4, slab, half)
            out.append(full_sum(scatter_sum(partial, a), b, along=True))
        return out

    def mapped_part(rows):
        (_, first), (_, second) = operator
        return dot(first, rows[0], precision=HIGH) + dot(second, rows[1], precision=HIGH)

    def col_sum(partial):
        return scatter_sum(partial.reshape(4, 2 * slab, half), "x")

    def twice_minus(new, old):
        return jax.tree.map(lambda a, b: 2.0 * a - b, new, old)

    def in_order(mine, other, axis):
        return jnp.concatenate([jnp.where(south, mine, other), jnp.where(south, other, mine)], axis=axis)

    def of_half(array, index, axis):
        size = array.shape[axis] // 2
        return lax.dynamic_slice_in_dim(array, index * size, size, axis)

    def gram_part(both):
        side = lax.dynamic_slice_in_dim(both, x * (width // 4), width // 4, 1)
        return dot(side, of_half(both, k, 1), 0, 0)

    def by_x(pieces):
        return jnp.concatenate([lax.dynamic_slice_in_dim(pieces, x ^ s, 1, 0) for s in range(4)])

    received = swap(of_half(start_vectors, 1 - k, 1), "k", 1)
    kept = of_half(start_vectors, k, 1)
    pair = in_order(kept, received, 0)
    pair = lax.ppermute(pair, CHIPS, TURN)

    other_matrix = swap(matrix, "k", 1)
    operator = [prepared(matrix, other_matrix, interval, where, h) for h in range(2)]
    pair, operator[0] = lax.optimization_barrier((pair, operator[0]))
    start = [gather(v, b) for v, (a, b) in zip((pair[:slab], pair[slab:]), orders)]
    start, operator[1] = lax.optimization_barrier((start, operator[1]))

    first = col_sum(mapped_part(gather_rows(start)))
    second = twice_minus(forward(gather_cols(first)), start)
    third = twice_minus(col_sum(mapped_part(gather_rows(second))), first)
    third_cols = gather_cols(third)

    part = gram_part(in_order(third_cols, swap(third_cols, "k", 1), 1))
    gram = gather(full_sum(full_sum(part, "y"), "z"), "x")
    gram = in_order(gram, swap(gram, "k", 1), 2)
    inverse = inverse_factor(gram, places, 1.0 / total_rows)

    first = forward(third_cols)
    second = twice_minus(col_sum(mapped_part(gather_rows(first))), third)
    third = twice_minus(forward(gather_cols(second)), first)
    mapped = mapped_part(gather_rows(third))

    final = jnp.concatenate([v[0] for v in third])
    final = lax.ppermute(final, CHIPS, TURN)
    final = gather_cols(final)
    final = dot(in_order(final, swap(final, "k", 1), 1), inverse, 1, 1)
    final_slab = lax.dynamic_slice_in_dim(final, k * slab, slab, 0)

    cross = by_x(dot(final, mapped, 0, 0).reshape(4, -1, half))
    mapped, cross = scatter_sum(jnp.stack([mapped.reshape(cross.shape), cross], 1), "x")
    part = jnp.stack([gram_part(final), cross])
    part = gather(full_sum(full_sum(part, "y"), "z"), "x")
    part = in_order(part, swap(part, "k", 1), 3)
    mapped_slab = in_order(of_half(mapped, k, 0), swap(of_half(mapped, 1 - k, 0), "k", 1), 1)
    mapped_slab = dot(mapped_slab, inverse, 1, 1)
    cross = dot(by_x(part[:, 1]).reshape(width, width) / total_rows, inverse, 1, 1)
    inverse = inverse_factor(part[:, 0], places, 1.0 / total_rows)

    projected = dot(dot(inverse, cross), inverse, 1, 1)
    basis = dot(final_slab, inverse, 1, 1)
    residual = dot(mapped_slab, inverse, 1, 1) - dot(basis, projected)
    return basis, projected, residual


def solution(mesh):
    torus = Mesh(mesh.devices.reshape(4, 2, 4, 4), ALL)
    placed = (P(ROW, COL), P(COL + ROW, None), P())
    return jax.shard_map(
        shards,
        mesh=torus,
        in_specs=placed,
        out_specs=(P(COL + ROW, None), P(), P(COL + ROW, None)),
        check_vma=False,
    )
```

```python
import functools

import jax
import jax.numpy as jnp
from jax import lax
from jax.experimental import pallas as pl
from jax.experimental.pallas import tpu as pltpu
from jax.sharding import Mesh
from jax.sharding import PartitionSpec as P


ALL = ("x", "k", "z", "y")
CHIPS = ("x", "z", "y")
ROW = ("x", "k")
COL = ("z", "y")


def dot(left, right, left_dim=1, right_dim=0):
    return lax.dot_general(
        left,
        right,
        (((left_dim,), (right_dim,)), ((), ())),
        precision=lax.Precision.HIGHEST,
        preferred_element_type=jnp.float32,
    )


def swap(array, axis, step):
    count = lax.axis_size(axis)
    return lax.ppermute(array, axis, [(i, i ^ step) for i in range(count)])


def swap_both(array, rider, axis, step):
    if rider is None:
        return swap(array, axis, step), None
    rows = array.size // array.shape[-1]
    sent = jnp.concatenate([array.reshape(rows, -1), rider])
    sent = swap(sent, axis, step)
    return sent[:rows].reshape(array.shape), sent[rows:]


def in_pairs(terms):
    while len(terms) > 1:
        terms = [a + b for a, b in zip(terms[::2], terms[1::2])]
    return terms[0]


def scatter_sum(pieces, axis, rider=None):
    total = pieces[0]
    riders = [rider]
    for step in range(1, pieces.shape[0]):
        term, extra = swap_both(pieces[step], rider, axis, step)
        total = total + term
        riders.append(extra)
    return total if rider is None else (total, riders)


def gather(piece, axis):
    count = lax.axis_size(axis)
    return jnp.stack([piece] + [swap(piece, axis, step) for step in range(1, count)])


def full_sum(piece, axis, rider=None):
    terms = [piece]
    riders = [rider]
    for step in range(1, lax.axis_size(axis)):
        term, extra = swap_both(piece, rider, axis, step)
        terms.append(term)
        riders.append(extra)
    return in_pairs(terms) if rider is None else (in_pairs(terms), in_pairs(riders))


def by_index(pieces, index):
    return jnp.concatenate([lax.dynamic_slice_in_dim(pieces, index ^ s, 1, 0) for s in range(4)])


def slab_at(step, where, half, inner):
    outer, inner = step // 2, 2 * (step % 2) + inner
    if half == 0:
        return (where[2] ^ outer) + 4 * inner
    return inner + 4 * (where[3] ^ outer)


def prepared_kernel(half, where_ref, ends_ref, *refs):
    *piece_refs, out_ref, turned_ref = refs
    x, k, z, y = (where_ref[i] for i in range(4))
    size, width = piece_refs[0].shape
    center = 0.5 * (ends_ref[0] + ends_ref[1])
    half_width = 0.5 * (ends_ref[1] - ends_ref[0])
    first_col = (4 * z + y) * width
    rows = lax.broadcasted_iota(jnp.int32, (size, 128), 0)
    lanes = lax.broadcasted_iota(jnp.int32, (size, 128), 1)
    for inner in range(2):
        slab = slab_at(pl.program_id(0), where_ref, half, inner)
        first_row = x * (32 * size) + slab * (2 * size) + half * size
        mine = slab // 8 == k
        for s in range(4):
            at = pl.multiple_of((x ^ s) * 128, 128)
            own = piece_refs[2 * inner][:, pl.ds(at, 128)]
            other = piece_refs[2 * inner + 1][:, pl.ds(at, 128)]
            values = jnp.where(mine, own, other)
            on = rows + first_row == lanes + (first_col + at)
            values = jnp.where(on, values - center, values) / half_width
            out_ref[size * inner : size * (inner + 1), 128 * s : 128 * (s + 1)] = values
    for s in range(4):
        turned_ref[128 * s : 128 * (s + 1), :] = out_ref[:, 128 * s : 128 * (s + 1)].T


def prepared(own, other, interval, where, half):
    rows, width = own.shape
    size = rows // 16
    pieces = [
        pl.BlockSpec((size, width), lambda i, w, e, n=n: ((2 * slab_at(i, w, half, n) + half) % 16, 0))
        for n in range(2)
    ]
    return pl.pallas_call(
        functools.partial(prepared_kernel, half),
        grid_spec=pltpu.PrefetchScalarGridSpec(
            num_scalar_prefetch=2,
            grid=(8,),
            in_specs=[pieces[0], pieces[0], pieces[1], pieces[1]],
            out_specs=[
                pl.BlockSpec((2 * size, width), lambda i, w, e: (i, 0)),
                pl.BlockSpec((width, 2 * size), lambda i, w, e: (0, i)),
            ],
        ),
        out_shape=[
            jax.ShapeDtypeStruct((rows, width), jnp.float32),
            jax.ShapeDtypeStruct((width, rows), jnp.float32),
        ],
        cost_estimate=pl.CostEstimate(flops=10**9, transcendentals=0, bytes_accessed=16 * rows * width),
    )(where, interval, own, other, own, other)


def panel(aug_ref, p):
    base = 16 * p
    rows = []
    for i in range(16):
        rows.append([
            jnp.broadcast_to(aug_ref[base + i : base + i + 1, :128], (8, 128)),
            jnp.broadcast_to(aug_ref[base + i : base + i + 1, 128:], (8, 128)),
        ])
    splat = {}
    for i in range(16):
        for j in range(i, 16):
            splat[i, j] = jnp.broadcast_to(rows[i][0][:, base + j : base + j + 1], (8, 128))
    for j in range(16):
        inv = lax.rsqrt(splat[j, j])
        u = {}
        for i in range(j + 1, 16):
            u[i] = splat[j, i] * inv
        for a in range(j + 1, 16):
            for b in range(a, 16):
                splat[a, b] = splat[a, b] - u[a] * u[b]
        for t in range(2):
            rows[j][t] = rows[j][t] * inv
        for i in range(j + 1, 16):
            for t in range(2):
                rows[i][t] = rows[i][t] - u[i] * rows[j][t]
    for i in range(16):
        for t in range(2):
            aug_ref[base + i : base + i + 1, 128 * t : 128 * t + 128] = rows[i][t][:1]


def factor_block(aug_ref):
    for p in range(8):
        panel(aug_ref, p)
        if p < 7:
            low = 16 * (p + 1)
            above = aug_ref[:low, :]
            rows = aug_ref[low : low + 16, :]
            aug_ref[low : low + 16, :] = rows - dot(above[:, low : low + 16], above, 0, 0)


def inverse_kernel(scale, place_ref, pieces_ref, out_ref, work_ref, aug_ref):
    count, size, n = pieces_ref.shape
    for i in range(count):
        at = pl.multiple_of(place_ref[i] * size, size)
        work_ref[pl.ds(at, size), :n] = pieces_ref[i] * scale
    rows = lax.broadcasted_iota(jnp.int32, (n, n), 0)
    lanes = lax.broadcasted_iota(jnp.int32, (n, n), 1)
    work_ref[:, n:] = jnp.where(rows == lanes, 1.0, 0.0)
    unit = jnp.where(rows[:128, :128] == lanes[:128, :128], 1.0, 0.0)

    def step(b, carry):
        at = pl.multiple_of(b * 128, 128)
        aug_ref[:, :128] = work_ref[pl.ds(at, 128), pl.ds(at, 128)]
        aug_ref[:, 128:] = unit
        factor_block(aug_ref)
        done = dot(aug_ref[:, 128:], work_ref[pl.ds(at, 128), :])
        out_ref[pl.ds(at, 128), :] = done[:, n:]
        later = jnp.where(lanes[:128] >= at + 128, done[:, :n], 0.0)
        work_ref[...] = work_ref[...] - dot(later, done, 0, 0)
        return carry

    lax.fori_loop(0, n // 128, step, 0)


def inverse_factor(pieces, place, scale):
    n = pieces.shape[-1]
    vmem = pl.BlockSpec(memory_space=pltpu.VMEM)
    return pl.pallas_call(
        functools.partial(inverse_kernel, scale),
        in_specs=[pl.BlockSpec(memory_space=pltpu.SMEM), vmem],
        out_specs=vmem,
        out_shape=jax.ShapeDtypeStruct((n, n), jnp.float32),
        scratch_shapes=[pltpu.VMEM((n, 2 * n), jnp.float32), pltpu.VMEM((128, 256), jnp.float32)],
        compiler_params=pltpu.CompilerParams(vmem_limit_bytes=24 * 2**20),
        cost_estimate=pl.CostEstimate(flops=6 * 10**9, transcendentals=n, bytes_accessed=8 * n * n),
    )(place, pieces)


def final_kernel(scale, place_ref, pieces_ref, cross_ref, block_ref, mapped_ref, *refs):
    basis_ref, projected_ref, residual_ref, inverse_ref, work_ref, aug_ref = refs
    inverse_kernel(scale, place_ref, pieces_ref, inverse_ref, work_ref, aug_ref)
    inverse = inverse_ref[...]
    projected_ref[...] = dot(dot(inverse, cross_ref[...]), inverse, 1, 1)
    basis_ref[...] = dot(block_ref[...], inverse, 1, 1)
    residual_ref[...] = dot(mapped_ref[...], inverse, 1, 1) - dot(basis_ref[...], projected_ref[...])


def final_results(pieces, place, cross, block, mapped, scale):
    n = pieces.shape[-1]
    vmem = pl.BlockSpec(memory_space=pltpu.VMEM)
    return pl.pallas_call(
        functools.partial(final_kernel, scale),
        in_specs=[pl.BlockSpec(memory_space=pltpu.SMEM), vmem, vmem, vmem, vmem],
        out_specs=[vmem, vmem, vmem],
        out_shape=[jax.ShapeDtypeStruct(a.shape, jnp.float32) for a in (block, cross, block)],
        scratch_shapes=[
            pltpu.VMEM((n, n), jnp.float32),
            pltpu.VMEM((n, 2 * n), jnp.float32),
            pltpu.VMEM((128, 256), jnp.float32),
        ],
        compiler_params=pltpu.CompilerParams(vmem_limit_bytes=32 * 2**20),
        cost_estimate=pl.CostEstimate(flops=8 * 10**9, transcendentals=n, bytes_accessed=16 * n * n),
    )(place, pieces, cross, block, mapped)


def turned(chip):
    return (chip // 4 % 4) * 16 + (chip // 16) * 4 + chip % 4


TURN = [(chip, turned(chip)) for chip in range(64)]


def shards(matrix, start_vectors, interval):
    slab, width = start_vectors.shape
    half = width // 2
    total_rows = slab * 128
    x, k, z, y = (lax.axis_index(a) for a in ALL)
    south = k == 0
    where = jnp.stack([x, k, z, y]).astype(jnp.int32)
    places = jnp.stack([x ^ s for s in range(4)]).astype(jnp.int32)

    orders = (("z", "y"), ("y", "z"))
    indices = (y, z)

    def gather_rows(fours):
        return [gather(v, a).reshape(16 * slab, half) for v, (a, b) in zip(fours, orders)]

    def gather_cols(pair):
        return gather(pair, "x").reshape(8 * slab, half)

    def partial_rows(cols):
        return [dot(plain, cols).reshape(4, 4, slab, half) for plain, across in operator]

    def forward(cols):
        return [full_sum(scatter_sum(v, a), b) for v, (a, b) in zip(partial_rows(cols), orders)]

    def mapped_part(rows):
        (_, first), (_, second) = operator
        return (dot(first, rows[0]) + dot(second, rows[1])).reshape(4, 2 * slab, half)

    def twice_minus(new, old):
        return jax.tree.map(lambda a, b: 2.0 * a - b, new, old)

    def in_order(mine, other, axis):
        return jnp.concatenate([jnp.where(south, mine, other), jnp.where(south, other, mine)], axis=axis)

    def of_half(array, index, axis):
        size = array.shape[axis] // 2
        return lax.dynamic_slice_in_dim(array, index * size, size, axis)

    def gram_part(both):
        side = lax.dynamic_slice_in_dim(both, x * (width // 4), width // 4, 1)
        return dot(side, of_half(both, k, 1), 0, 0)

    received = swap(of_half(start_vectors, 1 - k, 1), "k", 1)
    kept = of_half(start_vectors, k, 1)
    pair = in_order(kept, received, 0)
    pair = lax.ppermute(pair, CHIPS, TURN)

    other_matrix = swap(matrix, "k", 1)
    operator = [prepared(matrix, other_matrix, interval, where, h) for h in range(2)]
    pair, operator[0] = lax.optimization_barrier((pair, operator[0]))
    start = [
        by_index(gather(v, b), i) for v, (a, b), i in zip((pair[:slab], pair[slab:]), orders, indices)
    ]
    start, operator[1] = lax.optimization_barrier((start, operator[1]))

    first = scatter_sum(mapped_part(gather_rows(start)), "x")
    second = twice_minus(forward(gather_cols(first)), start)
    third = twice_minus(scatter_sum(mapped_part(gather_rows(second)), "x"), first)
    third_cols = gather_cols(third)

    gram = gram_part(in_order(third_cols, swap(third_cols, "k", 1), 1))
    partial = partial_rows(third_cols)
    early = full_sum(scatter_sum(partial[0], "z"), "y")
    late, gram = scatter_sum(partial[1], "y", gram)
    late, gram = full_sum(late, "z", in_pairs(gram))
    first = [early, late]
    mapped, gram = scatter_sum(mapped_part(gather_rows(first)), "x", gram)
    second = twice_minus(mapped, third)
    gram = jnp.stack(gram)
    gram = in_order(gram, swap(gram, "k", 1), 2)
    inverse = inverse_factor(gram, places, 1.0 / total_rows)
    third = twice_minus(forward(gather_cols(second)), first)
    mapped = mapped_part(gather_rows(third))

    final = [lax.dynamic_index_in_dim(v, i, 0, keepdims=False) for v, i in zip(third, indices)]
    final = lax.ppermute(jnp.concatenate(final), CHIPS, TURN)
    final = gather_cols(final)
    final = dot(in_order(final, swap(final, "k", 1), 1), inverse, 1, 1)
    final_slab = lax.dynamic_slice_in_dim(final, k * slab, slab, 0)

    cross = by_index(dot(final, mapped.reshape(8 * slab, half), 0, 0).reshape(4, -1, half), x)
    mapped, cross = scatter_sum(jnp.stack([mapped.reshape(cross.shape), cross], 1), "x")
    part = jnp.stack([gram_part(final), cross])
    part = gather(full_sum(full_sum(part, "y"), "z"), "x")
    part = in_order(part, swap(part, "k", 1), 3)
    mapped_slab = in_order(of_half(mapped, k, 0), swap(of_half(mapped, 1 - k, 0), "k", 1), 1)
    mapped_slab = dot(mapped_slab, inverse, 1, 1)
    cross = dot(by_index(part[:, 1], x).reshape(width, width) / total_rows, inverse, 1, 1)
    return tuple(final_results(part[:, 0], places, cross, final_slab, mapped_slab, 1.0 / total_rows))


def solution(mesh):
    torus = Mesh(mesh.devices.reshape(4, 2, 4, 4), ALL)
    placed = (P(ROW, COL), P(COL + ROW, None), P())
    return jax.shard_map(
        shards,
        mesh=torus,
        in_specs=placed,
        out_specs=(P(COL + ROW, None), P(), P(COL + ROW, None)),
        check_vma=False,
    )
```

```python
import functools

import jax
import jax.numpy as jnp
from jax import lax
from jax.experimental import pallas as pl
from jax.experimental.pallas import tpu as pltpu
from jax.sharding import Mesh
from jax.sharding import PartitionSpec as P


ALL = ("x", "k", "z", "y")
CHIPS = ("x", "z", "y")
ROW = ("x", "k")
COL = ("z", "y")


def dot(left, right, left_dim=1, right_dim=0):
    return lax.dot_general(
        left,
        right,
        (((left_dim,), (right_dim,)), ((), ())),
        precision=lax.Precision.HIGHEST,
        preferred_element_type=jnp.float32,
    )


def swap(array, axis, step):
    count = lax.axis_size(axis)
    return lax.ppermute(array, axis, [(i, i ^ step) for i in range(count)])


def swap_both(array, rider, axis, step):
    if rider is None:
        return swap(array, axis, step), None
    rows = array.size // array.shape[-1]
    sent = jnp.concatenate([array.reshape(rows, -1), rider])
    sent = swap(sent, axis, step)
    return sent[:rows].reshape(array.shape), sent[rows:]


def in_pairs(terms):
    while len(terms) > 1:
        terms = [a + b for a, b in zip(terms[::2], terms[1::2])]
    return terms[0]


def scatter_sum(pieces, axis, rider=None):
    total = pieces[0]
    riders = [rider]
    for step in range(1, pieces.shape[0]):
        term, extra = swap_both(pieces[step], rider, axis, step)
        total = total + term
        riders.append(extra)
    return total if rider is None else (total, riders)


def gather(piece, axis):
    count = lax.axis_size(axis)
    return jnp.stack([piece] + [swap(piece, axis, step) for step in range(1, count)])


def full_sum(piece, axis, rider=None):
    terms = [piece]
    riders = [rider]
    for step in range(1, lax.axis_size(axis)):
        term, extra = swap_both(piece, rider, axis, step)
        terms.append(term)
        riders.append(extra)
    return in_pairs(terms) if rider is None else (in_pairs(terms), in_pairs(riders))


def by_index(pieces, index):
    return jnp.concatenate([lax.dynamic_slice_in_dim(pieces, index ^ s, 1, 0) for s in range(4)])


def slab_at(step, where, half, inner):
    outer, inner = step // 2, 2 * (step % 2) + inner
    if half == 0:
        return (where[2] ^ outer) + 4 * inner
    return inner + 4 * (where[3] ^ outer)


def prepared_kernel(half, where_ref, ends_ref, *refs):
    *piece_refs, out_ref, turned_ref = refs
    x, k, z, y = (where_ref[i] for i in range(4))
    size, width = piece_refs[0].shape
    center = 0.5 * (ends_ref[0] + ends_ref[1])
    half_width = 0.5 * (ends_ref[1] - ends_ref[0])
    first_col = (4 * z + y) * width
    rows = lax.broadcasted_iota(jnp.int32, (size, 128), 0)
    lanes = lax.broadcasted_iota(jnp.int32, (size, 128), 1)
    for inner in range(2):
        slab = slab_at(pl.program_id(0), where_ref, half, inner)
        first_row = x * (32 * size) + slab * (2 * size) + half * size
        mine = slab // 8 == k
        for s in range(4):
            at = pl.multiple_of((x ^ s) * 128, 128)
            own = piece_refs[2 * inner][:, pl.ds(at, 128)]
            other = piece_refs[2 * inner + 1][:, pl.ds(at, 128)]
            values = jnp.where(mine, own, other)
            on = rows + first_row == lanes + (first_col + at)
            values = jnp.where(on, values - center, values) / half_width
            out_ref[size * inner : size * (inner + 1), 128 * s : 128 * (s + 1)] = values
    for s in range(4):
        turned_ref[128 * s : 128 * (s + 1), :] = out_ref[:, 128 * s : 128 * (s + 1)].T


def prepared(own, other, interval, where, half):
    rows, width = own.shape
    size = rows // 16
    pieces = [
        pl.BlockSpec((size, width), lambda i, w, e, n=n: ((2 * slab_at(i, w, half, n) + half) % 16, 0))
        for n in range(2)
    ]
    return pl.pallas_call(
        functools.partial(prepared_kernel, half),
        grid_spec=pltpu.PrefetchScalarGridSpec(
            num_scalar_prefetch=2,
            grid=(8,),
            in_specs=[pieces[0], pieces[0], pieces[1], pieces[1]],
            out_specs=[
                pl.BlockSpec((2 * size, width), lambda i, w, e: (i, 0)),
                pl.BlockSpec((width, 2 * size), lambda i, w, e: (0, i)),
            ],
        ),
        out_shape=[
            jax.ShapeDtypeStruct((rows, width), jnp.float32),
            jax.ShapeDtypeStruct((width, rows), jnp.float32),
        ],
        cost_estimate=pl.CostEstimate(flops=10**9, transcendentals=0, bytes_accessed=16 * rows * width),
    )(where, interval, own, other, own, other)


def panel(aug_ref, p):
    base = 16 * p
    rows = []
    for i in range(16):
        rows.append([
            jnp.broadcast_to(aug_ref[base + i : base + i + 1, :128], (8, 128)),
            jnp.broadcast_to(aug_ref[base + i : base + i + 1, 128:], (8, 128)),
        ])
    splat = {}
    for i in range(16):
        for j in range(i, 16):
            splat[i, j] = jnp.broadcast_to(rows[i][0][:, base + j : base + j + 1], (8, 128))
    for j in range(16):
        inv = lax.rsqrt(splat[j, j])
        u = {}
        for i in range(j + 1, 16):
            u[i] = splat[j, i] * inv
        for a in range(j + 1, 16):
            for b in range(a, 16):
                splat[a, b] = splat[a, b] - u[a] * u[b]
        for t in range(2):
            rows[j][t] = rows[j][t] * inv
        for i in range(j + 1, 16):
            for t in range(2):
                rows[i][t] = rows[i][t] - u[i] * rows[j][t]
    for i in range(16):
        for t in range(2):
            aug_ref[base + i : base + i + 1, 128 * t : 128 * t + 128] = rows[i][t][:1]


def factor_block(aug_ref):
    for p in range(8):
        panel(aug_ref, p)
        if p < 7:
            low = 16 * (p + 1)
            above = aug_ref[:low, :]
            rows = aug_ref[low : low + 16, :]
            aug_ref[low : low + 16, :] = rows - dot(above[:, low : low + 16], above, 0, 0)


def inverse_kernel(scale, place_ref, pieces_ref, out_ref, work_ref, aug_ref, done_ref):
    count, size, n = pieces_ref.shape
    for i in range(count):
        at = pl.multiple_of(place_ref[i] * size, size)
        work_ref[pl.ds(at, size), :n] = pieces_ref[i] * scale
    rows = lax.broadcasted_iota(jnp.int32, (n, n), 0)
    lanes = lax.broadcasted_iota(jnp.int32, (n, n), 1)
    work_ref[:, n:] = jnp.where(rows == lanes, 1.0, 0.0)
    unit = jnp.where(rows[:128, :128] == lanes[:128, :128], 1.0, 0.0)

    def step(b, carry):
        at = pl.multiple_of(b * 128, 128)
        aug_ref[:, :128] = work_ref[pl.ds(at, 128), pl.ds(at, 128)]
        aug_ref[:, 128:] = unit
        factor_block(aug_ref)
        done = dot(aug_ref[:, 128:], work_ref[pl.ds(at, 128), :])
        out_ref[pl.ds(at, 128), :] = done[:, n:]
        done_ref[...] = done

        def below(i, carry):
            low = pl.multiple_of(i * 128, 128)
            done = done_ref[...]
            work_ref[pl.ds(low, 128), :] -= dot(done_ref[:, pl.ds(low, 128)], done, 0, 0)
            return carry

        lax.fori_loop(b + 1, n // 128, below, 0)
        return carry

    lax.fori_loop(0, n // 128, step, 0)


def factor_scratch(n):
    return [pltpu.VMEM(shape, jnp.float32) for shape in ((n, 2 * n), (128, 256), (128, 2 * n))]


def inverse_factor(pieces, place, scale):
    n = pieces.shape[-1]
    vmem = pl.BlockSpec(memory_space=pltpu.VMEM)
    return pl.pallas_call(
        functools.partial(inverse_kernel, scale),
        in_specs=[pl.BlockSpec(memory_space=pltpu.SMEM), vmem],
        out_specs=vmem,
        out_shape=jax.ShapeDtypeStruct((n, n), jnp.float32),
        scratch_shapes=factor_scratch(n),
        compiler_params=pltpu.CompilerParams(vmem_limit_bytes=24 * 2**20),
        cost_estimate=pl.CostEstimate(flops=6 * 10**9, transcendentals=n, bytes_accessed=8 * n * n),
    )(place, pieces)


def final_kernel(inverse_ref, cross_ref, block_ref, mapped_ref, basis_ref, projected_ref, residual_ref):
    inverse = inverse_ref[...]
    projected_ref[...] = dot(dot(inverse, cross_ref[...]), inverse, 1, 1)
    basis_ref[...] = dot(block_ref[...], inverse, 1, 1)
    residual_ref[...] = dot(mapped_ref[...], inverse, 1, 1) - dot(basis_ref[...], projected_ref[...])


def final_results(inverse, cross, block, mapped):
    n = cross.shape[0]
    vmem = pl.BlockSpec(memory_space=pltpu.VMEM)
    return pl.pallas_call(
        final_kernel,
        in_specs=[vmem] * 4,
        out_specs=[vmem] * 3,
        out_shape=[jax.ShapeDtypeStruct(a.shape, jnp.float32) for a in (block, cross, block)],
        compiler_params=pltpu.CompilerParams(vmem_limit_bytes=24 * 2**20),
        cost_estimate=pl.CostEstimate(flops=2 * 10**9, transcendentals=0, bytes_accessed=16 * n * n),
    )(inverse, cross, block, mapped)


def turned(chip):
    return (chip // 4 % 4) * 16 + (chip // 16) * 4 + chip % 4


TURN = [(chip, turned(chip)) for chip in range(64)]


def shards(matrix, start_vectors, interval):
    slab, width = start_vectors.shape
    half = width // 2
    total_rows = slab * 128
    x, k, z, y = (lax.axis_index(a) for a in ALL)
    south = k == 0
    where = jnp.stack([x, k, z, y]).astype(jnp.int32)
    places = jnp.stack([x ^ s for s in range(4)]).astype(jnp.int32)

    orders = (("z", "y"), ("y", "z"))
    indices = (y, z)

    def gather_rows(fours):
        return [gather(v, a).reshape(16 * slab, half) for v, (a, b) in zip(fours, orders)]

    def gather_cols(pair):
        return gather(pair, "x").reshape(8 * slab, half)

    def partial_rows(cols):
        return [dot(plain, cols).reshape(4, 4, slab, half) for plain, across in operator]

    def forward(cols):
        return [full_sum(scatter_sum(v, a), b) for v, (a, b) in zip(partial_rows(cols), orders)]

    def mapped_part(rows):
        (_, first), (_, second) = operator
        return (dot(first, rows[0]) + dot(second, rows[1])).reshape(4, 2 * slab, half)

    def twice_minus(new, old):
        return jax.tree.map(lambda a, b: 2.0 * a - b, new, old)

    def in_order(mine, other, axis):
        return jnp.concatenate([jnp.where(south, mine, other), jnp.where(south, other, mine)], axis=axis)

    def of_half(array, index, axis):
        size = array.shape[axis] // 2
        return lax.dynamic_slice_in_dim(array, index * size, size, axis)

    def gram_part(both):
        side = lax.dynamic_slice_in_dim(both, x * (width // 4), width // 4, 1)
        return dot(side, of_half(both, k, 1), 0, 0)

    received = swap(of_half(start_vectors, 1 - k, 1), "k", 1)
    kept = of_half(start_vectors, k, 1)
    pair = in_order(kept, received, 0)
    pair = lax.ppermute(pair, CHIPS, TURN)

    other_matrix = swap(matrix, "k", 1)
    pair, first_half = lax.optimization_barrier((pair, prepared(matrix, other_matrix, interval, where, 0)))
    start = [
        by_index(gather(v, b), i) for v, (a, b), i in zip((pair[:slab], pair[slab:]), orders, indices)
    ]
    start, where = lax.optimization_barrier((start, where))
    operator = [first_half, prepared(matrix, other_matrix, interval, where, 1)]

    first = scatter_sum(mapped_part(gather_rows(start)), "x")
    second = twice_minus(forward(gather_cols(first)), start)
    third = twice_minus(scatter_sum(mapped_part(gather_rows(second)), "x"), first)
    third_cols = gather_cols(third)

    gram = gram_part(in_order(third_cols, swap(third_cols, "k", 1), 1))
    partial = partial_rows(third_cols)
    early = full_sum(scatter_sum(partial[0], "z"), "y")
    late, gram = scatter_sum(partial[1], "y", gram)
    late, gram = full_sum(late, "z", in_pairs(gram))
    first = [early, late]
    mapped, gram = scatter_sum(mapped_part(gather_rows(first)), "x", gram)
    second = twice_minus(mapped, third)
    gram = jnp.stack(gram)
    gram = in_order(gram, swap(gram, "k", 1), 2)
    third = twice_minus(forward(gather_cols(second)), first)
    mapped = mapped_part(gather_rows(third))

    final = [lax.dynamic_index_in_dim(v, i, 0, keepdims=False) for v, i in zip(third, indices)]
    final = lax.ppermute(jnp.concatenate(final), CHIPS, TURN)
    final, gram = lax.optimization_barrier((final, gram))
    inverse = inverse_factor(gram, places, 1.0 / total_rows)
    final = gather_cols(final)
    final = dot(in_order(final, swap(final, "k", 1), 1), inverse, 1, 1)
    final_slab = lax.dynamic_slice_in_dim(final, k * slab, slab, 0)

    gram = gather(full_sum(full_sum(gram_part(final), "y"), "z"), "x")
    gram = in_order(gram, swap(gram, "k", 1), 2)
    cross = by_index(dot(final, mapped.reshape(8 * slab, half), 0, 0).reshape(4, -1, half), x)
    mapped, cross = scatter_sum(jnp.stack([mapped.reshape(cross.shape), cross], 1), "x")
    cross = full_sum(full_sum(cross, "y"), "z")
    cross = by_index(gather(cross, "x"), x).reshape(width, half)
    cross = in_order(cross, swap(cross, "k", 1), 1) / total_rows
    mapped_slab = in_order(of_half(mapped, k, 0), swap(of_half(mapped, 1 - k, 0), "k", 1), 1)
    cross, mapped_slab = dot(cross, inverse, 1, 1), dot(mapped_slab, inverse, 1, 1)
    inverse = inverse_factor(gram, places, 1.0 / total_rows)
    return tuple(final_results(inverse, cross, final_slab, mapped_slab))


def solution(mesh):
    torus = Mesh(mesh.devices.reshape(4, 2, 4, 4), ALL)
    placed = (P(ROW, COL), P(COL + ROW, None), P())
    return jax.shard_map(
        shards,
        mesh=torus,
        in_specs=placed,
        out_specs=(P(COL + ROW, None), P(), P(COL + ROW, None)),
        check_vma=False,
    )
```

```python
import functools

import jax
import jax.numpy as jnp
from jax import lax
from jax.experimental import pallas as pl
from jax.experimental.pallas import tpu as pltpu
from jax.sharding import Mesh
from jax.sharding import PartitionSpec as P


ALL = ("x", "k", "z", "y")
CHIPS = ("x", "z", "y")
ROW = ("x", "k")
COL = ("z", "y")


def dot(left, right, left_dim=1, right_dim=0):
    return lax.dot_general(
        left,
        right,
        (((left_dim,), (right_dim,)), ((), ())),
        precision=lax.Precision.HIGHEST,
        preferred_element_type=jnp.float32,
    )


def swap(array, axis, step):
    count = lax.axis_size(axis)
    return lax.ppermute(array, axis, [(i, i ^ step) for i in range(count)])


def scatter_sum(pieces, axis):
    total = pieces[0]
    for step in range(1, pieces.shape[0]):
        total = total + swap(pieces[step], axis, step)
    return total


def gather(piece, axis):
    count = lax.axis_size(axis)
    return jnp.stack([piece] + [swap(piece, axis, step) for step in range(1, count)])


def full_sum(piece, axis):
    terms = [piece] + [swap(piece, axis, step) for step in range(1, lax.axis_size(axis))]
    while len(terms) > 1:
        terms = [a + b for a, b in zip(terms[::2], terms[1::2])]
    return terms[0]


def by_index(pieces, index):
    return jnp.concatenate([lax.dynamic_slice_in_dim(pieces, index ^ s, 1, 0) for s in range(4)])


def slab_at(step, where, half, inner):
    outer, inner = step // 2, 2 * (step % 2) + inner
    if half == 0:
        return (where[2] ^ outer) + 4 * inner
    return inner + 4 * (where[3] ^ outer)


def prepared_kernel(half, where_ref, ends_ref, *refs):
    *piece_refs, out_ref, turned_ref = refs
    x, k, z, y = (where_ref[i] for i in range(4))
    size, width = piece_refs[0].shape
    center = 0.5 * (ends_ref[0] + ends_ref[1])
    half_width = 0.5 * (ends_ref[1] - ends_ref[0])
    first_col = (4 * z + y) * width
    rows = lax.broadcasted_iota(jnp.int32, (size, 128), 0)
    lanes = lax.broadcasted_iota(jnp.int32, (size, 128), 1)
    for inner in range(2):
        slab = slab_at(pl.program_id(0), where_ref, half, inner)
        first_row = x * (32 * size) + slab * (2 * size) + half * size
        mine = slab // 8 == k
        for s in range(4):
            at = pl.multiple_of((x ^ s) * 128, 128)
            own = piece_refs[2 * inner][:, pl.ds(at, 128)]
            other = piece_refs[2 * inner + 1][:, pl.ds(at, 128)]
            values = jnp.where(mine, own, other)
            on = rows + first_row == lanes + (first_col + at)
            values = jnp.where(on, values - center, values) / half_width
            out_ref[size * inner : size * (inner + 1), 128 * s : 128 * (s + 1)] = values
    for s in range(4):
        turned_ref[128 * s : 128 * (s + 1), :] = out_ref[:, 128 * s : 128 * (s + 1)].T


def prepared(own, other, interval, where, half):
    rows, width = own.shape
    size = rows // 16
    pieces = [
        pl.BlockSpec((size, width), lambda i, w, e, n=n: ((2 * slab_at(i, w, half, n) + half) % 16, 0))
        for n in range(2)
    ]
    return pl.pallas_call(
        functools.partial(prepared_kernel, half),
        grid_spec=pltpu.PrefetchScalarGridSpec(
            num_scalar_prefetch=2,
            grid=(8,),
            in_specs=[pieces[0], pieces[0], pieces[1], pieces[1]],
            out_specs=[
                pl.BlockSpec((2 * size, width), lambda i, w, e: (i, 0)),
                pl.BlockSpec((width, 2 * size), lambda i, w, e: (0, i)),
            ],
        ),
        out_shape=[
            jax.ShapeDtypeStruct((rows, width), jnp.float32),
            jax.ShapeDtypeStruct((width, rows), jnp.float32),
        ],
        cost_estimate=pl.CostEstimate(flops=10**9, transcendentals=0, bytes_accessed=16 * rows * width),
    )(where, interval, own, other, own, other)


def panel(aug_ref, p):
    base = 16 * p
    rows = []
    for i in range(16):
        rows.append([
            jnp.broadcast_to(aug_ref[base + i : base + i + 1, :128], (8, 128)),
            jnp.broadcast_to(aug_ref[base + i : base + i + 1, 128:], (8, 128)),
        ])
    splat = {}
    for i in range(16):
        for j in range(i, 16):
            splat[i, j] = jnp.broadcast_to(rows[i][0][:, base + j : base + j + 1], (8, 128))
    for j in range(16):
        inv = lax.rsqrt(splat[j, j])
        u = {}
        for i in range(j + 1, 16):
            u[i] = splat[j, i] * inv
        for a in range(j + 1, 16):
            for b in range(a, 16):
                splat[a, b] = splat[a, b] - u[a] * u[b]
        for t in range(2):
            rows[j][t] = rows[j][t] * inv
        for i in range(j + 1, 16):
            for t in range(2):
                rows[i][t] = rows[i][t] - u[i] * rows[j][t]
    for i in range(16):
        for t in range(2):
            aug_ref[base + i : base + i + 1, 128 * t : 128 * t + 128] = rows[i][t][:1]


def factor_block(aug_ref):
    for p in range(8):
        panel(aug_ref, p)
        if p < 7:
            low = 16 * (p + 1)
            above = aug_ref[:low, :]
            rows = aug_ref[low : low + 16, :]
            aug_ref[low : low + 16, :] = rows - dot(above[:, low : low + 16], above, 0, 0)


def inverse_kernel(scale, place_ref, pieces_ref, out_ref, work_ref, aug_ref, done_ref):
    count, size, n = pieces_ref.shape
    for i in range(count):
        at = pl.multiple_of(place_ref[i] * size, size)
        work_ref[pl.ds(at, size), :n] = pieces_ref[i] * scale
    rows = lax.broadcasted_iota(jnp.int32, (n, n), 0)
    lanes = lax.broadcasted_iota(jnp.int32, (n, n), 1)
    work_ref[:, n:] = jnp.where(rows == lanes, 1.0, 0.0)
    unit = jnp.where(rows[:128, :128] == lanes[:128, :128], 1.0, 0.0)

    def step(b, carry):
        at = pl.multiple_of(b * 128, 128)
        aug_ref[:, :128] = work_ref[pl.ds(at, 128), pl.ds(at, 128)]
        aug_ref[:, 128:] = unit
        factor_block(aug_ref)
        done = dot(aug_ref[:, 128:], work_ref[pl.ds(at, 128), :])
        out_ref[pl.ds(at, 128), :] = done[:, n:]
        done_ref[...] = done

        def below(i, carry):
            low = pl.multiple_of(i * 128, 128)
            done = done_ref[...]
            work_ref[pl.ds(low, 128), :] -= dot(done_ref[:, pl.ds(low, 128)], done, 0, 0)
            return carry

        lax.fori_loop(b + 1, n // 128, below, 0)
        return carry

    lax.fori_loop(0, n // 128, step, 0)


def factor_scratch(n):
    return [pltpu.VMEM(shape, jnp.float32) for shape in ((n, 2 * n), (128, 256), (128, 2 * n))]


def inverse_factor(pieces, place, scale):
    n = pieces.shape[-1]
    vmem = pl.BlockSpec(memory_space=pltpu.VMEM)
    return pl.pallas_call(
        functools.partial(inverse_kernel, scale),
        in_specs=[pl.BlockSpec(memory_space=pltpu.SMEM), vmem],
        out_specs=vmem,
        out_shape=jax.ShapeDtypeStruct((n, n), jnp.float32),
        scratch_shapes=factor_scratch(n),
        compiler_params=pltpu.CompilerParams(vmem_limit_bytes=24 * 2**20),
        cost_estimate=pl.CostEstimate(flops=6 * 10**9, transcendentals=n, bytes_accessed=8 * n * n),
    )(place, pieces)


def final_kernel(inverse_ref, cross_ref, block_ref, mapped_ref, basis_ref, projected_ref, residual_ref):
    inverse = inverse_ref[...]
    projected_ref[...] = dot(dot(inverse, cross_ref[...]), inverse, 1, 1)
    basis_ref[...] = dot(block_ref[...], inverse, 1, 1)
    residual_ref[...] = dot(mapped_ref[...], inverse, 1, 1) - dot(basis_ref[...], projected_ref[...])


def final_results(inverse, cross, block, mapped):
    n = cross.shape[0]
    vmem = pl.BlockSpec(memory_space=pltpu.VMEM)
    return pl.pallas_call(
        final_kernel,
        in_specs=[vmem] * 4,
        out_specs=[vmem] * 3,
        out_shape=[jax.ShapeDtypeStruct(a.shape, jnp.float32) for a in (block, cross, block)],
        compiler_params=pltpu.CompilerParams(vmem_limit_bytes=24 * 2**20),
        cost_estimate=pl.CostEstimate(flops=2 * 10**9, transcendentals=0, bytes_accessed=16 * n * n),
    )(inverse, cross, block, mapped)


def turned(chip):
    return (chip // 4 % 4) * 16 + (chip // 16) * 4 + chip % 4


TURN = [(chip, turned(chip)) for chip in range(64)]


def shards(matrix, start_vectors, interval):
    slab, width = start_vectors.shape
    half = width // 2
    total_rows = slab * 128
    x, k, z, y = (lax.axis_index(a) for a in ALL)
    south = k == 0
    where = jnp.stack([x, k, z, y]).astype(jnp.int32)
    places = jnp.stack([x ^ s for s in range(4)]).astype(jnp.int32)

    orders = (("z", "y"), ("y", "z"))
    indices = (y, z)

    def gather_rows(fours):
        return [gather(v, a).reshape(16 * slab, half) for v, (a, b) in zip(fours, orders)]

    def gather_cols(pair):
        return gather(pair, "x").reshape(8 * slab, half)

    def partial_rows(cols):
        return [dot(plain, cols).reshape(4, 4, slab, half) for plain, across in operator]

    def forward(cols):
        return [full_sum(scatter_sum(v, a), b) for v, (a, b) in zip(partial_rows(cols), orders)]

    def mapped_part(rows):
        (_, first), (_, second) = operator
        return (dot(first, rows[0]) + dot(second, rows[1])).reshape(4, 2 * slab, half)

    def twice_minus(new, old):
        return jax.tree.map(lambda a, b: 2.0 * a - b, new, old)

    def in_order(mine, other, axis):
        return jnp.concatenate([jnp.where(south, mine, other), jnp.where(south, other, mine)], axis=axis)

    def of_half(array, index, axis):
        size = array.shape[axis] // 2
        return lax.dynamic_slice_in_dim(array, index * size, size, axis)

    def gram_part(both):
        side = lax.dynamic_slice_in_dim(both, x * (width // 4), width // 4, 1)
        return dot(side, of_half(both, k, 1), 0, 0)

    received = swap(of_half(start_vectors, 1 - k, 1), "k", 1)
    kept = of_half(start_vectors, k, 1)
    pair = in_order(kept, received, 0)
    pair = lax.ppermute(pair, CHIPS, TURN)

    matrix, received = lax.optimization_barrier((matrix, received))
    other_matrix = swap(matrix, "k", 1)
    pair, first_half = lax.optimization_barrier((pair, prepared(matrix, other_matrix, interval, where, 0)))
    start = [
        by_index(gather(v, b), i) for v, (a, b), i in zip((pair[:slab], pair[slab:]), orders, indices)
    ]
    start, where = lax.optimization_barrier((start, where))
    operator = [first_half, prepared(matrix, other_matrix, interval, where, 1)]

    first = scatter_sum(mapped_part(gather_rows(start)), "x")
    second = twice_minus(forward(gather_cols(first)), start)
    third = twice_minus(scatter_sum(mapped_part(gather_rows(second)), "x"), first)
    third_cols = gather_cols(third)

    first = forward(third_cols)
    gram = gram_part(in_order(third_cols, swap(third_cols, "k", 1), 1))
    mapped, gram = lax.optimization_barrier((mapped_part(gather_rows(first)), gram))
    gram = full_sum(gram, "y")
    second = twice_minus(scatter_sum(mapped, "x"), third)
    second, gram = lax.optimization_barrier((second, gram))
    gram = full_sum(gram, "z")
    partial, gram = lax.optimization_barrier((partial_rows(gather_cols(second)), gram))
    gram = gather(gram, "x")
    third = [full_sum(scatter_sum(v, a), b) for v, (a, b) in zip(partial, orders)]
    third = twice_minus(third, first)
    gram = in_order(gram, swap(gram, "k", 1), 2)
    mapped = mapped_part(gather_rows(third))

    final = [lax.dynamic_index_in_dim(v, i, 0, keepdims=False) for v, i in zip(third, indices)]
    final = lax.ppermute(jnp.concatenate(final), CHIPS, TURN)
    final, gram = lax.optimization_barrier((final, gram))
    inverse = inverse_factor(gram, places, 1.0 / total_rows)
    final = gather_cols(final)
    final = dot(in_order(final, swap(final, "k", 1), 1), inverse, 1, 1)
    final_slab = lax.dynamic_slice_in_dim(final, k * slab, slab, 0)

    gram = gather(full_sum(full_sum(gram_part(final), "y"), "z"), "x")
    gram = in_order(gram, swap(gram, "k", 1), 2)
    cross = by_index(dot(final, mapped.reshape(8 * slab, half), 0, 0).reshape(4, -1, half), x)
    mapped, cross = scatter_sum(jnp.stack([mapped.reshape(cross.shape), cross], 1), "x")
    cross = full_sum(full_sum(cross, "y"), "z")
    cross = by_index(gather(cross, "x"), x).reshape(width, half)
    cross = in_order(cross, swap(cross, "k", 1), 1) / total_rows
    mapped_slab = in_order(of_half(mapped, k, 0), swap(of_half(mapped, 1 - k, 0), "k", 1), 1)
    cross, mapped_slab = dot(cross, inverse, 1, 1), dot(mapped_slab, inverse, 1, 1)
    inverse = inverse_factor(gram, places, 1.0 / total_rows)
    return tuple(final_results(inverse, cross, final_slab, mapped_slab))


def solution(mesh):
    torus = Mesh(mesh.devices.reshape(4, 2, 4, 4), ALL)
    placed = (P(ROW, COL), P(COL + ROW, None), P())
    return jax.shard_map(
        shards,
        mesh=torus,
        in_specs=placed,
        out_specs=(P(COL + ROW, None), P(), P(COL + ROW, None)),
        check_vma=False,
    )
```

```python
import functools

import jax
import jax.numpy as jnp
from jax import lax
from jax.experimental import pallas as pl
from jax.experimental.pallas import tpu as pltpu
from jax.sharding import Mesh
from jax.sharding import PartitionSpec as P


ALL = ("x", "k", "z", "y")
CHIPS = ("x", "z", "y")
ROW = ("x", "k")
COL = ("z", "y")


def dot(left, right, left_dim=1, right_dim=0):
    return lax.dot_general(
        left,
        right,
        (((left_dim,), (right_dim,)), ((), ())),
        precision=lax.Precision.HIGHEST,
        preferred_element_type=jnp.float32,
    )


def swap(array, axis, step):
    count = lax.axis_size(axis)
    return lax.ppermute(array, axis, [(i, i ^ step) for i in range(count)])


def scatter_sum(pieces, axis):
    total = pieces[0]
    for step in range(1, pieces.shape[0]):
        total = total + swap(pieces[step], axis, step)
    return total


def gather(piece, axis):
    count = lax.axis_size(axis)
    return jnp.stack([piece] + [swap(piece, axis, step) for step in range(1, count)])


def full_sum(piece, axis):
    terms = [piece] + [swap(piece, axis, step) for step in range(1, lax.axis_size(axis))]
    while len(terms) > 1:
        terms = [a + b for a, b in zip(terms[::2], terms[1::2])]
    return terms[0]


def by_index(pieces, index):
    return jnp.concatenate([lax.dynamic_slice_in_dim(pieces, index ^ s, 1, 0) for s in range(4)])


def slab_at(step, where, half, inner):
    outer, inner = step // 2, 2 * (step % 2) + inner
    if half == 0:
        return (where[2] ^ outer) + 4 * inner
    return inner + 4 * (where[3] ^ outer)


def prepared_kernel(half, where_ref, ends_ref, *refs):
    *piece_refs, out_ref, turned_ref = refs
    x, k, z, y = (where_ref[i] for i in range(4))
    size, width = piece_refs[0].shape
    center = 0.5 * (ends_ref[0] + ends_ref[1])
    half_width = 0.5 * (ends_ref[1] - ends_ref[0])
    first_col = (4 * z + y) * width
    rows = lax.broadcasted_iota(jnp.int32, (size, 128), 0)
    lanes = lax.broadcasted_iota(jnp.int32, (size, 128), 1)
    for inner in range(2):
        slab = slab_at(pl.program_id(0), where_ref, half, inner)
        first_row = x * (32 * size) + slab * (2 * size) + half * size
        mine = slab // 8 == k
        for s in range(4):
            at = pl.multiple_of((x ^ s) * 128, 128)
            own = piece_refs[2 * inner][:, pl.ds(at, 128)]
            other = piece_refs[2 * inner + 1][:, pl.ds(at, 128)]
            values = jnp.where(mine, own, other)
            on = rows + first_row == lanes + (first_col + at)
            values = jnp.where(on, values - center, values) / half_width
            out_ref[size * inner : size * (inner + 1), 128 * s : 128 * (s + 1)] = values
    for s in range(4):
        turned_ref[128 * s : 128 * (s + 1), :] = out_ref[:, 128 * s : 128 * (s + 1)].T


def prepared(own, other, interval, where, half):
    rows, width = own.shape
    size = rows // 16
    pieces = [
        pl.BlockSpec((size, width), lambda i, w, e, n=n: ((2 * slab_at(i, w, half, n) + half) % 16, 0))
        for n in range(2)
    ]
    return pl.pallas_call(
        functools.partial(prepared_kernel, half),
        grid_spec=pltpu.PrefetchScalarGridSpec(
            num_scalar_prefetch=2,
            grid=(8,),
            in_specs=[pieces[0], pieces[0], pieces[1], pieces[1]],
            out_specs=[
                pl.BlockSpec((2 * size, width), lambda i, w, e: (i, 0)),
                pl.BlockSpec((width, 2 * size), lambda i, w, e: (0, i)),
            ],
        ),
        out_shape=[
            jax.ShapeDtypeStruct((rows, width), jnp.float32),
            jax.ShapeDtypeStruct((width, rows), jnp.float32),
        ],
        cost_estimate=pl.CostEstimate(flops=10**9, transcendentals=0, bytes_accessed=16 * rows * width),
    )(where, interval, own, other, own, other)


def panel(aug_ref, p):
    base = 16 * p
    rows = []
    for i in range(16):
        rows.append([
            jnp.broadcast_to(aug_ref[base + i : base + i + 1, :128], (8, 128)),
            jnp.broadcast_to(aug_ref[base + i : base + i + 1, 128:], (8, 128)),
        ])
    splat = {}
    for i in range(16):
        for j in range(i, 16):
            splat[i, j] = jnp.broadcast_to(rows[i][0][:, base + j : base + j + 1], (8, 128))
    for j in range(16):
        inv = lax.rsqrt(splat[j, j])
        u = {}
        for i in range(j + 1, 16):
            u[i] = splat[j, i] * inv
        for a in range(j + 1, 16):
            for b in range(a, 16):
                splat[a, b] = splat[a, b] - u[a] * u[b]
        for t in range(2):
            rows[j][t] = rows[j][t] * inv
        for i in range(j + 1, 16):
            for t in range(2):
                rows[i][t] = rows[i][t] - u[i] * rows[j][t]
    for i in range(16):
        for t in range(2):
            aug_ref[base + i : base + i + 1, 128 * t : 128 * t + 128] = rows[i][t][:1]


def factor_block(aug_ref):
    for p in range(8):
        panel(aug_ref, p)
        if p < 7:
            low = 16 * (p + 1)
            above = aug_ref[:low, :]
            rows = aug_ref[low : low + 16, :]
            aug_ref[low : low + 16, :] = rows - dot(above[:, low : low + 16], above, 0, 0)


def factor_rows(first, last, out_ref, work_ref, aug_ref, done_ref):
    n = work_ref.shape[0]
    rows = lax.broadcasted_iota(jnp.int32, (128, 128), 0)
    lanes = lax.broadcasted_iota(jnp.int32, (128, 128), 1)
    unit = jnp.where(rows == lanes, 1.0, 0.0)

    def step(b, carry):
        at = pl.multiple_of(b * 128, 128)
        aug_ref[:, :128] = work_ref[pl.ds(at, 128), pl.ds(at, 128)]
        aug_ref[:, 128:] = unit
        factor_block(aug_ref)
        done = dot(aug_ref[:, 128:], work_ref[pl.ds(at, 128), :])
        out_ref[pl.ds(at, 128), :] = done[:, n:]
        done_ref[...] = done

        def below(i, carry):
            low = pl.multiple_of(i * 128, 128)
            done = done_ref[...]
            work_ref[pl.ds(low, 128), :] -= dot(done_ref[:, pl.ds(low, 128)], done, 0, 0)
            return carry

        lax.fori_loop(b + 1, n // 128, below, 0)
        return carry

    lax.fori_loop(first, last, step, 0)


def set_up(scale, place_ref, pieces_ref, work_ref):
    count, size, n = pieces_ref.shape
    for i in range(count):
        at = pl.multiple_of(place_ref[i] * size, size)
        work_ref[pl.ds(at, size), :n] = pieces_ref[i] * scale
    rows = lax.broadcasted_iota(jnp.int32, (n, n), 0)
    lanes = lax.broadcasted_iota(jnp.int32, (n, n), 1)
    work_ref[:, n:] = jnp.where(rows == lanes, 1.0, 0.0)


def inverse_kernel(scale, place_ref, pieces_ref, out_ref, work_ref, *scratch):
    set_up(scale, place_ref, pieces_ref, work_ref)
    factor_rows(0, work_ref.shape[0] // 128, out_ref, work_ref, *scratch)


def upper_kernel(scale, place_ref, pieces_ref, out_ref, rest_ref, full_ref, work_ref, *scratch):
    set_up(scale, place_ref, pieces_ref, work_ref)
    top = out_ref.shape[0]
    factor_rows(0, top // 128, full_ref, work_ref, *scratch)
    out_ref[...] = full_ref[:top, :]
    rest_ref[...] = work_ref[top:, :]


def lower_kernel(top_ref, rest_ref, out_ref, work_ref, *scratch):
    top = top_ref.shape[0]
    out_ref[:top, :] = top_ref[...]
    work_ref[top:, :] = rest_ref[...]
    factor_rows(top // 128, work_ref.shape[0] // 128, out_ref, work_ref, *scratch)


def factor_scratch(n):
    return [pltpu.VMEM(shape, jnp.float32) for shape in ((n, 2 * n), (128, 256), (128, 2 * n))]


VMEM = pl.BlockSpec(memory_space=pltpu.VMEM)
SMEM = pl.BlockSpec(memory_space=pltpu.SMEM)


def factor_call(kernel, ins, outs, n, extra=()):
    return pl.pallas_call(
        kernel,
        in_specs=ins,
        out_specs=[VMEM] * len(outs),
        out_shape=[jax.ShapeDtypeStruct(shape, jnp.float32) for shape in outs],
        scratch_shapes=[*extra, *factor_scratch(n)],
        compiler_params=pltpu.CompilerParams(vmem_limit_bytes=24 * 2**20),
        cost_estimate=pl.CostEstimate(flops=6 * 10**9 // len(outs), transcendentals=n, bytes_accessed=8 * n * n),
    )


def inverse_factor(pieces, place, scale):
    n = pieces.shape[-1]
    return factor_call(functools.partial(inverse_kernel, scale), [SMEM, VMEM], [(n, n)], n)(place, pieces)[0]


def inverse_upper(pieces, place, scale):
    n = pieces.shape[-1]
    outs = [(n // 2, n), (n // 2, 2 * n)]
    extra = [pltpu.VMEM((n, n), jnp.float32)]
    return factor_call(functools.partial(upper_kernel, scale), [SMEM, VMEM], outs, n, extra)(place, pieces)


def inverse_lower(top, rest):
    n = top.shape[-1]
    return factor_call(lower_kernel, [VMEM, VMEM], [(n, n)], n)(top, rest)[0]


def final_kernel(inverse_ref, cross_ref, block_ref, mapped_ref, basis_ref, projected_ref, residual_ref):
    inverse = inverse_ref[...]
    projected_ref[...] = dot(dot(inverse, cross_ref[...]), inverse, 1, 1)
    basis_ref[...] = dot(block_ref[...], inverse, 1, 1)
    residual_ref[...] = dot(mapped_ref[...], inverse, 1, 1) - dot(basis_ref[...], projected_ref[...])


def final_results(inverse, cross, block, mapped):
    n = cross.shape[0]
    vmem = pl.BlockSpec(memory_space=pltpu.VMEM)
    return pl.pallas_call(
        final_kernel,
        in_specs=[vmem] * 4,
        out_specs=[vmem] * 3,
        out_shape=[jax.ShapeDtypeStruct(a.shape, jnp.float32) for a in (block, cross, block)],
        compiler_params=pltpu.CompilerParams(vmem_limit_bytes=24 * 2**20),
        cost_estimate=pl.CostEstimate(flops=2 * 10**9, transcendentals=0, bytes_accessed=16 * n * n),
    )(inverse, cross, block, mapped)


def turned(chip):
    return (chip // 4 % 4) * 16 + (chip // 16) * 4 + chip % 4


TURN = [(chip, turned(chip)) for chip in range(64)]


def shards(matrix, start_vectors, interval):
    slab, width = start_vectors.shape
    half = width // 2
    total_rows = slab * 128
    x, k, z, y = (lax.axis_index(a) for a in ALL)
    south = k == 0
    where = jnp.stack([x, k, z, y]).astype(jnp.int32)
    places = jnp.stack([x ^ s for s in range(4)]).astype(jnp.int32)

    orders = (("z", "y"), ("y", "z"))
    indices = (y, z)

    def gather_rows(fours):
        return [gather(v, a).reshape(16 * slab, half) for v, (a, b) in zip(fours, orders)]

    def gather_cols(pair):
        return gather(pair, "x").reshape(8 * slab, half)

    def partial_rows(cols):
        return [dot(plain, cols).reshape(4, 4, slab, half) for plain, across in operator]

    def forward(cols):
        return [full_sum(scatter_sum(v, a), b) for v, (a, b) in zip(partial_rows(cols), orders)]

    def mapped_part(rows):
        (_, first), (_, second) = operator
        return (dot(first, rows[0]) + dot(second, rows[1])).reshape(4, 2 * slab, half)

    def twice_minus(new, old):
        return jax.tree.map(lambda a, b: 2.0 * a - b, new, old)

    def in_order(mine, other, axis):
        return jnp.concatenate([jnp.where(south, mine, other), jnp.where(south, other, mine)], axis=axis)

    def of_half(array, index, axis):
        size = array.shape[axis] // 2
        return lax.dynamic_slice_in_dim(array, index * size, size, axis)

    def gram_part(both):
        side = lax.dynamic_slice_in_dim(both, x * (width // 4), width // 4, 1)
        return dot(side, of_half(both, k, 1), 0, 0)

    received = swap(of_half(start_vectors, 1 - k, 1), "k", 1)
    kept = of_half(start_vectors, k, 1)
    pair = in_order(kept, received, 0)
    pair = lax.ppermute(pair, CHIPS, TURN)

    matrix, received = lax.optimization_barrier((matrix, received))
    other_matrix = swap(matrix, "k", 1)
    pair, first_half = lax.optimization_barrier((pair, prepared(matrix, other_matrix, interval, where, 0)))
    start = [
        by_index(gather(v, b), i) for v, (a, b), i in zip((pair[:slab], pair[slab:]), orders, indices)
    ]
    start, where = lax.optimization_barrier((start, where))
    operator = [first_half, prepared(matrix, other_matrix, interval, where, 1)]

    first = scatter_sum(mapped_part(gather_rows(start)), "x")
    second = twice_minus(forward(gather_cols(first)), start)
    third = twice_minus(scatter_sum(mapped_part(gather_rows(second)), "x"), first)
    third_cols = gather_cols(third)

    first = forward(third_cols)
    gram = gram_part(in_order(third_cols, swap(third_cols, "k", 1), 1))
    mapped, gram = lax.optimization_barrier((mapped_part(gather_rows(first)), gram))
    gram = full_sum(gram, "y")
    second = twice_minus(scatter_sum(mapped, "x"), third)
    second, gram = lax.optimization_barrier((second, gram))
    gram = full_sum(gram, "z")
    partial, gram = lax.optimization_barrier((partial_rows(gather_cols(second)), gram))
    gram = gather(gram, "x")
    third = [full_sum(scatter_sum(v, a), b) for v, (a, b) in zip(partial, orders)]
    third = twice_minus(third, first)
    gram = in_order(gram, swap(gram, "k", 1), 2)
    mapped = mapped_part(gather_rows(third))

    final = [lax.dynamic_index_in_dim(v, i, 0, keepdims=False) for v, i in zip(third, indices)]
    final = lax.ppermute(jnp.concatenate(final), CHIPS, TURN)
    upper = inverse_upper(gram, places, 1.0 / total_rows)
    final, upper = lax.optimization_barrier((final, upper))
    final = gather_cols(final)
    inverse = inverse_lower(*upper)
    final = dot(in_order(final, swap(final, "k", 1), 1), inverse, 1, 1)
    final_slab = lax.dynamic_slice_in_dim(final, k * slab, slab, 0)

    gram = gather(full_sum(full_sum(gram_part(final), "y"), "z"), "x")
    gram = in_order(gram, swap(gram, "k", 1), 2)
    cross = by_index(dot(final, mapped.reshape(8 * slab, half), 0, 0).reshape(4, -1, half), x)
    mapped, cross = scatter_sum(jnp.stack([mapped.reshape(cross.shape), cross], 1), "x")
    cross = full_sum(full_sum(cross, "y"), "z")
    cross = by_index(gather(cross, "x"), x).reshape(width, half)
    cross = in_order(cross, swap(cross, "k", 1), 1) / total_rows
    mapped_slab = in_order(of_half(mapped, k, 0), swap(of_half(mapped, 1 - k, 0), "k", 1), 1)
    cross, mapped_slab = dot(cross, inverse, 1, 1), dot(mapped_slab, inverse, 1, 1)
    inverse = inverse_factor(gram, places, 1.0 / total_rows)
    return tuple(final_results(inverse, cross, final_slab, mapped_slab))


def solution(mesh):
    torus = Mesh(mesh.devices.reshape(4, 2, 4, 4), ALL)
    placed = (P(ROW, COL), P(COL + ROW, None), P())
    return jax.shard_map(
        shards,
        mesh=torus,
        in_specs=placed,
        out_specs=(P(COL + ROW, None), P(), P(COL + ROW, None)),
        check_vma=False,
    )
```

```python
import functools

import jax
import jax.numpy as jnp
from jax import lax
from jax.experimental import pallas as pl
from jax.experimental.pallas import tpu as pltpu
from jax.sharding import Mesh
from jax.sharding import PartitionSpec as P


ALL = ("x", "k", "z", "y")
CHIPS = ("x", "z", "y")
ROW = ("x", "k")
COL = ("z", "y")


def dot(left, right, left_dim=1, right_dim=0):
    return lax.dot_general(
        left,
        right,
        (((left_dim,), (right_dim,)), ((), ())),
        precision=lax.Precision.HIGHEST,
        preferred_element_type=jnp.float32,
    )


def swap(array, axis, step):
    count = lax.axis_size(axis)
    return lax.ppermute(array, axis, [(i, i ^ step) for i in range(count)])


def scatter_sum(pieces, axis):
    total = pieces[0]
    for step in range(1, pieces.shape[0]):
        total = total + swap(pieces[step], axis, step)
    return total


def gather(piece, axis):
    count = lax.axis_size(axis)
    return jnp.stack([piece] + [swap(piece, axis, step) for step in range(1, count)])


def full_sum(piece, axis):
    terms = [piece] + [swap(piece, axis, step) for step in range(1, lax.axis_size(axis))]
    while len(terms) > 1:
        terms = [a + b for a, b in zip(terms[::2], terms[1::2])]
    return terms[0]


def by_index(pieces, index):
    return jnp.concatenate([lax.dynamic_slice_in_dim(pieces, index ^ s, 1, 0) for s in range(4)])


def slab_at(step, where, half, inner):
    outer, inner = step // 2, 2 * (step % 2) + inner
    if half == 0:
        return (where[2] ^ outer) + 4 * inner
    return inner + 4 * (where[3] ^ outer)


def prepared_kernel(half, where_ref, ends_ref, *refs):
    *piece_refs, out_ref, turned_ref = refs
    x, k, z, y = (where_ref[i] for i in range(4))
    size, width = piece_refs[0].shape
    center = 0.5 * (ends_ref[0] + ends_ref[1])
    half_width = 0.5 * (ends_ref[1] - ends_ref[0])
    first_col = (4 * z + y) * width
    rows = lax.broadcasted_iota(jnp.int32, (size, 128), 0)
    lanes = lax.broadcasted_iota(jnp.int32, (size, 128), 1)
    for inner in range(2):
        slab = slab_at(pl.program_id(0), where_ref, half, inner)
        first_row = x * (32 * size) + slab * (2 * size) + half * size
        mine = slab // 8 == k
        for s in range(4):
            at = pl.multiple_of((x ^ s) * 128, 128)
            own = piece_refs[2 * inner][:, pl.ds(at, 128)]
            other = piece_refs[2 * inner + 1][:, pl.ds(at, 128)]
            values = jnp.where(mine, own, other)
            on = rows + first_row == lanes + (first_col + at)
            values = jnp.where(on, values - center, values) / half_width
            out_ref[size * inner : size * (inner + 1), 128 * s : 128 * (s + 1)] = values
    for s in range(4):
        turned_ref[128 * s : 128 * (s + 1), :] = out_ref[:, 128 * s : 128 * (s + 1)].T


def prepared(own, other, interval, where, half):
    rows, width = own.shape
    size = rows // 16
    pieces = [
        pl.BlockSpec((size, width), lambda i, w, e, n=n: ((2 * slab_at(i, w, half, n) + half) % 16, 0))
        for n in range(2)
    ]
    return pl.pallas_call(
        functools.partial(prepared_kernel, half),
        grid_spec=pltpu.PrefetchScalarGridSpec(
            num_scalar_prefetch=2,
            grid=(8,),
            in_specs=[pieces[0], pieces[0], pieces[1], pieces[1]],
            out_specs=[
                pl.BlockSpec((2 * size, width), lambda i, w, e: (i, 0)),
                pl.BlockSpec((width, 2 * size), lambda i, w, e: (0, i)),
            ],
        ),
        out_shape=[
            jax.ShapeDtypeStruct((rows, width), jnp.float32),
            jax.ShapeDtypeStruct((width, rows), jnp.float32),
        ],
        cost_estimate=pl.CostEstimate(flops=10**9, transcendentals=0, bytes_accessed=16 * rows * width),
    )(where, interval, own, other, own, other)


def panel(aug_ref, p):
    base = 16 * p
    rows = []
    for i in range(16):
        rows.append([
            jnp.broadcast_to(aug_ref[base + i : base + i + 1, :128], (8, 128)),
            jnp.broadcast_to(aug_ref[base + i : base + i + 1, 128:], (8, 128)),
        ])
    splat = {}
    for i in range(16):
        for j in range(i, 16):
            splat[i, j] = jnp.broadcast_to(rows[i][0][:, base + j : base + j + 1], (8, 128))
    for j in range(16):
        inv = lax.rsqrt(splat[j, j])
        u = {}
        for i in range(j + 1, 16):
            u[i] = splat[j, i] * inv
        for a in range(j + 1, 16):
            for b in range(a, 16):
                splat[a, b] = splat[a, b] - u[a] * u[b]
        for t in range(2):
            rows[j][t] = rows[j][t] * inv
        for i in range(j + 1, 16):
            for t in range(2):
                rows[i][t] = rows[i][t] - u[i] * rows[j][t]
    for i in range(16):
        for t in range(2):
            aug_ref[base + i : base + i + 1, 128 * t : 128 * t + 128] = rows[i][t][:1]


def factor_block(aug_ref):
    for p in range(8):
        panel(aug_ref, p)
        if p < 7:
            low = 16 * (p + 1)
            above = aug_ref[:low, :]
            rows = aug_ref[low : low + 16, :]
            aug_ref[low : low + 16, :] = rows - dot(above[:, low : low + 16], above, 0, 0)


def factor_rows(first, last, out_ref, work_ref, aug_ref, done_ref):
    n = work_ref.shape[0]
    rows = lax.broadcasted_iota(jnp.int32, (128, 128), 0)
    lanes = lax.broadcasted_iota(jnp.int32, (128, 128), 1)
    unit = jnp.where(rows == lanes, 1.0, 0.0)

    def step(b, carry):
        at = pl.multiple_of(b * 128, 128)
        aug_ref[:, :128] = work_ref[pl.ds(at, 128), pl.ds(at, 128)]
        aug_ref[:, 128:] = unit
        factor_block(aug_ref)
        done = dot(aug_ref[:, 128:], work_ref[pl.ds(at, 128), :])
        out_ref[pl.ds(at, 128), :] = done[:, n:]
        done_ref[...] = done

        def below(i, carry):
            low = pl.multiple_of(i * 128, 128)
            done = done_ref[...]
            work_ref[pl.ds(low, 128), :] -= dot(done_ref[:, pl.ds(low, 128)], done, 0, 0)
            return carry

        lax.fori_loop(b + 1, n // 128, below, 0)
        return carry

    lax.fori_loop(first, last, step, 0)


def set_up(scale, place_ref, pieces_ref, work_ref):
    count, size, n = pieces_ref.shape
    for i in range(count):
        at = pl.multiple_of(place_ref[i] * size, size)
        work_ref[pl.ds(at, size), :n] = pieces_ref[i] * scale
    rows = lax.broadcasted_iota(jnp.int32, (n, n), 0)
    lanes = lax.broadcasted_iota(jnp.int32, (n, n), 1)
    work_ref[:, n:] = jnp.where(rows == lanes, 1.0, 0.0)


def inverse_kernel(scale, place_ref, pieces_ref, out_ref, work_ref, *scratch):
    set_up(scale, place_ref, pieces_ref, work_ref)
    factor_rows(0, work_ref.shape[0] // 128, out_ref, work_ref, *scratch)


def upper_kernel(scale, place_ref, pieces_ref, out_ref, rest_ref, full_ref, work_ref, *scratch):
    set_up(scale, place_ref, pieces_ref, work_ref)
    top = out_ref.shape[0]
    factor_rows(0, top // 128, full_ref, work_ref, *scratch)
    out_ref[...] = full_ref[:top, :]
    rest_ref[...] = work_ref[top:, :]


def lower_kernel(top_ref, rest_ref, out_ref, work_ref, *scratch):
    top = top_ref.shape[0]
    out_ref[:top, :] = top_ref[...]
    work_ref[top:, :] = rest_ref[...]
    factor_rows(top // 128, work_ref.shape[0] // 128, out_ref, work_ref, *scratch)


def factor_scratch(n):
    return [pltpu.VMEM(shape, jnp.float32) for shape in ((n, 2 * n), (128, 256), (128, 2 * n))]


VMEM = pl.BlockSpec(memory_space=pltpu.VMEM)
SMEM = pl.BlockSpec(memory_space=pltpu.SMEM)


def factor_call(kernel, ins, outs, n, extra=()):
    return pl.pallas_call(
        kernel,
        in_specs=ins,
        out_specs=[VMEM] * len(outs),
        out_shape=[jax.ShapeDtypeStruct(shape, jnp.float32) for shape in outs],
        scratch_shapes=[*extra, *factor_scratch(n)],
        compiler_params=pltpu.CompilerParams(vmem_limit_bytes=24 * 2**20),
        cost_estimate=pl.CostEstimate(flops=6 * 10**9 // len(outs), transcendentals=n, bytes_accessed=8 * n * n),
    )


def inverse_factor(pieces, place, scale):
    n = pieces.shape[-1]
    return factor_call(functools.partial(inverse_kernel, scale), [SMEM, VMEM], [(n, n)], n)(place, pieces)[0]


def inverse_upper(pieces, place, scale):
    n = pieces.shape[-1]
    outs = [(n // 2, n), (n // 2, 2 * n)]
    extra = [pltpu.VMEM((n, n), jnp.float32)]
    return factor_call(functools.partial(upper_kernel, scale), [SMEM, VMEM], outs, n, extra)(place, pieces)


def inverse_lower(top, rest):
    n = top.shape[-1]
    return factor_call(lower_kernel, [VMEM, VMEM], [(n, n)], n)(top, rest)[0]


def final_kernel(inverse_ref, cross_ref, block_ref, mapped_ref, basis_ref, projected_ref, residual_ref):
    inverse = inverse_ref[...]
    projected_ref[...] = dot(dot(inverse, cross_ref[...]), inverse, 1, 1)
    basis_ref[...] = dot(block_ref[...], inverse, 1, 1)
    residual_ref[...] = dot(mapped_ref[...], inverse, 1, 1) - dot(basis_ref[...], projected_ref[...])


def final_results(inverse, cross, block, mapped):
    n = cross.shape[0]
    vmem = pl.BlockSpec(memory_space=pltpu.VMEM)
    return pl.pallas_call(
        final_kernel,
        in_specs=[vmem] * 4,
        out_specs=[vmem] * 3,
        out_shape=[jax.ShapeDtypeStruct(a.shape, jnp.float32) for a in (block, cross, block)],
        compiler_params=pltpu.CompilerParams(vmem_limit_bytes=24 * 2**20),
        cost_estimate=pl.CostEstimate(flops=2 * 10**9, transcendentals=0, bytes_accessed=16 * n * n),
    )(inverse, cross, block, mapped)


def turned(chip):
    return (chip // 4 % 4) * 16 + (chip // 16) * 4 + chip % 4


TURN = [(chip, turned(chip)) for chip in range(64)]


def shards(matrix, start_vectors, interval):
    slab, width = start_vectors.shape
    half = width // 2
    total_rows = slab * 128
    x, k, z, y = (lax.axis_index(a) for a in ALL)
    south = k == 0
    where = jnp.stack([x, k, z, y]).astype(jnp.int32)
    places = jnp.stack([x ^ s for s in range(4)]).astype(jnp.int32)

    orders = (("z", "y"), ("y", "z"))
    indices = (y, z)

    def gather_rows(fours):
        return [gather(v, a).reshape(16 * slab, half) for v, (a, b) in zip(fours, orders)]

    def gather_cols(pair):
        return gather(pair, "x").reshape(8 * slab, half)

    def partial_rows(cols):
        return [dot(plain, cols).reshape(4, 4, slab, half) for plain, across in operator]

    def forward(cols):
        return [full_sum(scatter_sum(v, a), b) for v, (a, b) in zip(partial_rows(cols), orders)]

    def mapped_part(rows):
        (_, first), (_, second) = operator
        return (dot(first, rows[0]) + dot(second, rows[1])).reshape(4, 2 * slab, half)

    def twice_minus(new, old):
        return jax.tree.map(lambda a, b: 2.0 * a - b, new, old)

    def in_order(mine, other, axis):
        return jnp.concatenate([jnp.where(south, mine, other), jnp.where(south, other, mine)], axis=axis)

    def of_half(array, index, axis):
        size = array.shape[axis] // 2
        return lax.dynamic_slice_in_dim(array, index * size, size, axis)

    def gram_part(both):
        side = lax.dynamic_slice_in_dim(both, x * (width // 4), width // 4, 1)
        return dot(side, of_half(both, k, 1), 0, 0)

    received = swap(of_half(start_vectors, 1 - k, 1), "k", 1)
    kept = of_half(start_vectors, k, 1)
    pair = in_order(kept, received, 0)
    pair = lax.ppermute(pair, CHIPS, TURN)

    matrix, received = lax.optimization_barrier((matrix, received))
    other_matrix = swap(matrix, "k", 1)
    pair, first_half = lax.optimization_barrier((pair, prepared(matrix, other_matrix, interval, where, 0)))
    start = [
        by_index(gather(v, b), i) for v, (a, b), i in zip((pair[:slab], pair[slab:]), orders, indices)
    ]
    start[1], where = lax.optimization_barrier((start[1], where))
    operator = [first_half, prepared(matrix, other_matrix, interval, where, 1)]

    first = scatter_sum(mapped_part(gather_rows(start)), "x")
    second = twice_minus(forward(gather_cols(first)), start)
    third = twice_minus(scatter_sum(mapped_part(gather_rows(second)), "x"), first)
    third_cols = gather_cols(third)

    first = forward(third_cols)
    gram = gram_part(in_order(third_cols, swap(third_cols, "k", 1), 1))
    mapped, gram = lax.optimization_barrier((mapped_part(gather_rows(first)), gram))
    gram = full_sum(gram, "y")
    second = twice_minus(scatter_sum(mapped, "x"), third)
    second, gram = lax.optimization_barrier((second, gram))
    gram = full_sum(gram, "z")
    partial = partial_rows(gather_cols(second))
    partial[1], gram = lax.optimization_barrier((partial[1], gram))
    gram = gather(gram, "x")
    third = [full_sum(scatter_sum(v, a), b) for v, (a, b) in zip(partial, orders)]
    third = twice_minus(third, first)
    gram = in_order(gram, swap(gram, "k", 1), 2)
    mapped = mapped_part(gather_rows(third))

    final = [lax.dynamic_index_in_dim(v, i, 0, keepdims=False) for v, i in zip(third, indices)]
    final = lax.ppermute(jnp.concatenate(final), CHIPS, TURN)
    upper = inverse_upper(gram, places, 1.0 / total_rows)
    final, upper = lax.optimization_barrier((final, upper))
    final = gather_cols(final)
    inverse = inverse_lower(*upper)
    final = dot(in_order(final, swap(final, "k", 1), 1), inverse, 1, 1)
    final_slab = lax.dynamic_slice_in_dim(final, k * slab, slab, 0)

    gram = gather(full_sum(full_sum(gram_part(final), "y"), "z"), "x")
    gram = in_order(gram, swap(gram, "k", 1), 2)
    cross = by_index(dot(final, mapped.reshape(8 * slab, half), 0, 0).reshape(4, -1, half), x)
    mapped, cross = scatter_sum(jnp.stack([mapped.reshape(cross.shape), cross], 1), "x")
    cross = full_sum(full_sum(cross, "y"), "z")
    cross = by_index(gather(cross, "x"), x).reshape(width, half)
    cross = in_order(cross, swap(cross, "k", 1), 1) / total_rows
    mapped_slab = in_order(of_half(mapped, k, 0), swap(of_half(mapped, 1 - k, 0), "k", 1), 1)
    cross, mapped_slab = dot(cross, inverse, 1, 1), dot(mapped_slab, inverse, 1, 1)
    inverse = inverse_factor(gram, places, 1.0 / total_rows)
    return tuple(final_results(inverse, cross, final_slab, mapped_slab))


def solution(mesh):
    torus = Mesh(mesh.devices.reshape(4, 2, 4, 4), ALL)
    placed = (P(ROW, COL), P(COL + ROW, None), P())
    return jax.shard_map(
        shards,
        mesh=torus,
        in_specs=placed,
        out_specs=(P(COL + ROW, None), P(), P(COL + ROW, None)),
        check_vma=False,
    )
```

```python
import functools

import jax
import jax.numpy as jnp
from jax import lax
from jax.experimental import pallas as pl
from jax.experimental.pallas import tpu as pltpu
from jax.sharding import Mesh
from jax.sharding import PartitionSpec as P


ALL = ("x", "k", "z", "y")
CHIPS = ("x", "z", "y")
ROW = ("x", "k")
COL = ("z", "y")


def dot(left, right, left_dim=1, right_dim=0):
    return lax.dot_general(
        left,
        right,
        (((left_dim,), (right_dim,)), ((), ())),
        precision=lax.Precision.HIGHEST,
        preferred_element_type=jnp.float32,
    )


def swap(array, axis, step):
    count = lax.axis_size(axis)
    return lax.ppermute(array, axis, [(i, i ^ step) for i in range(count)])


def scatter_sum(pieces, axis):
    total = pieces[0]
    for step in range(1, pieces.shape[0]):
        total = total + swap(pieces[step], axis, step)
    return total


def gather(piece, axis):
    count = lax.axis_size(axis)
    return jnp.stack([piece] + [swap(piece, axis, step) for step in range(1, count)])


def full_sum(piece, axis):
    terms = [piece] + [swap(piece, axis, step) for step in range(1, lax.axis_size(axis))]
    while len(terms) > 1:
        terms = [a + b for a, b in zip(terms[::2], terms[1::2])]
    return terms[0]


def by_index(pieces, index):
    return jnp.concatenate([lax.dynamic_slice_in_dim(pieces, index ^ s, 1, 0) for s in range(4)])


def slab_at(step, where, half, inner):
    outer, inner = step // 2, 2 * (step % 2) + inner
    if half == 0:
        return (where[2] ^ outer) + 4 * inner
    return inner + 4 * (where[3] ^ outer)


def prepared_kernel(half, where_ref, ends_ref, *refs):
    *piece_refs, out_ref, turned_ref = refs
    x, k, z, y = (where_ref[i] for i in range(4))
    size, width = piece_refs[0].shape
    center = 0.5 * (ends_ref[0] + ends_ref[1])
    half_width = 0.5 * (ends_ref[1] - ends_ref[0])
    first_col = (4 * z + y) * width
    rows = lax.broadcasted_iota(jnp.int32, (size, 128), 0)
    lanes = lax.broadcasted_iota(jnp.int32, (size, 128), 1)
    for inner in range(2):
        slab = slab_at(pl.program_id(0), where_ref, half, inner)
        first_row = x * (32 * size) + slab * (2 * size) + half * size
        mine = slab // 8 == k
        for s in range(4):
            at = pl.multiple_of((x ^ s) * 128, 128)
            own = piece_refs[2 * inner][:, pl.ds(at, 128)]
            other = piece_refs[2 * inner + 1][:, pl.ds(at, 128)]
            values = jnp.where(mine, own, other)
            on = rows + first_row == lanes + (first_col + at)
            values = jnp.where(on, values - center, values) / half_width
            out_ref[size * inner : size * (inner + 1), 128 * s : 128 * (s + 1)] = values
    for s in range(4):
        turned_ref[128 * s : 128 * (s + 1), :] = out_ref[:, 128 * s : 128 * (s + 1)].T


def prepared(own, other, interval, where, half):
    rows, width = own.shape
    size = rows // 16
    pieces = [
        pl.BlockSpec((size, width), lambda i, w, e, n=n: ((2 * slab_at(i, w, half, n) + half) % 16, 0))
        for n in range(2)
    ]
    return pl.pallas_call(
        functools.partial(prepared_kernel, half),
        grid_spec=pltpu.PrefetchScalarGridSpec(
            num_scalar_prefetch=2,
            grid=(8,),
            in_specs=[pieces[0], pieces[0], pieces[1], pieces[1]],
            out_specs=[
                pl.BlockSpec((2 * size, width), lambda i, w, e: (i, 0)),
                pl.BlockSpec((width, 2 * size), lambda i, w, e: (0, i)),
            ],
        ),
        out_shape=[
            jax.ShapeDtypeStruct((rows, width), jnp.float32),
            jax.ShapeDtypeStruct((width, rows), jnp.float32),
        ],
        cost_estimate=pl.CostEstimate(flops=10**9, transcendentals=0, bytes_accessed=16 * rows * width),
    )(where, interval, own, other, own, other)


def panel(aug_ref, p):
    base = 16 * p
    rows = []
    for i in range(16):
        rows.append([
            jnp.broadcast_to(aug_ref[base + i : base + i + 1, :128], (8, 128)),
            jnp.broadcast_to(aug_ref[base + i : base + i + 1, 128:], (8, 128)),
        ])
    splat = {}
    for i in range(16):
        for j in range(i, 16):
            splat[i, j] = jnp.broadcast_to(rows[i][0][:, base + j : base + j + 1], (8, 128))
    for j in range(16):
        inv = lax.rsqrt(splat[j, j])
        u = {}
        for i in range(j + 1, 16):
            u[i] = splat[j, i] * inv
        for a in range(j + 1, 16):
            for b in range(a, 16):
                splat[a, b] = splat[a, b] - u[a] * u[b]
        for t in range(2):
            rows[j][t] = rows[j][t] * inv
        for i in range(j + 1, 16):
            for t in range(2):
                rows[i][t] = rows[i][t] - u[i] * rows[j][t]
    for i in range(16):
        for t in range(2):
            aug_ref[base + i : base + i + 1, 128 * t : 128 * t + 128] = rows[i][t][:1]


def factor_block(aug_ref):
    for p in range(8):
        panel(aug_ref, p)
        if p < 7:
            low = 16 * (p + 1)
            above = aug_ref[:low, :]
            rows = aug_ref[low : low + 16, :]
            aug_ref[low : low + 16, :] = rows - dot(above[:, low : low + 16], above, 0, 0)


def factor_rows(first, last, out_ref, work_ref, aug_ref, done_ref):
    n = work_ref.shape[0]
    rows = lax.broadcasted_iota(jnp.int32, (128, 128), 0)
    lanes = lax.broadcasted_iota(jnp.int32, (128, 128), 1)
    unit = jnp.where(rows == lanes, 1.0, 0.0)

    def step(b, carry):
        at = pl.multiple_of(b * 128, 128)
        aug_ref[:, :128] = work_ref[pl.ds(at, 128), pl.ds(at, 128)]
        aug_ref[:, 128:] = unit
        factor_block(aug_ref)
        done = dot(aug_ref[:, 128:], work_ref[pl.ds(at, 128), :])
        out_ref[pl.ds(at, 128), :] = done[:, n:]
        done_ref[...] = done

        def below(i, carry):
            low = pl.multiple_of(i * 128, 128)
            done = done_ref[...]
            work_ref[pl.ds(low, 128), :] -= dot(done_ref[:, pl.ds(low, 128)], done, 0, 0)
            return carry

        lax.fori_loop(b + 1, n // 128, below, 0)
        return carry

    lax.fori_loop(first, last, step, 0)


def set_up(scale, place_ref, pieces_ref, work_ref):
    count, size, n = pieces_ref.shape
    for i in range(count):
        at = pl.multiple_of(place_ref[i] * size, size)
        work_ref[pl.ds(at, size), :n] = pieces_ref[i] * scale
    rows = lax.broadcasted_iota(jnp.int32, (n, n), 0)
    lanes = lax.broadcasted_iota(jnp.int32, (n, n), 1)
    work_ref[:, n:] = jnp.where(rows == lanes, 1.0, 0.0)


def inverse_kernel(scale, place_ref, pieces_ref, out_ref, work_ref, *scratch):
    set_up(scale, place_ref, pieces_ref, work_ref)
    factor_rows(0, work_ref.shape[0] // 128, out_ref, work_ref, *scratch)


def upper_kernel(scale, place_ref, pieces_ref, out_ref, rest_ref, full_ref, work_ref, *scratch):
    set_up(scale, place_ref, pieces_ref, work_ref)
    top = out_ref.shape[0]
    factor_rows(0, top // 128, full_ref, work_ref, *scratch)
    out_ref[...] = full_ref[:top, :]
    rest_ref[...] = work_ref[top:, :]


def lower_kernel(top_ref, rest_ref, out_ref, work_ref, *scratch):
    top = top_ref.shape[0]
    out_ref[:top, :] = top_ref[...]
    work_ref[top:, :] = rest_ref[...]
    factor_rows(top // 128, work_ref.shape[0] // 128, out_ref, work_ref, *scratch)


def factor_scratch(n):
    return [pltpu.VMEM(shape, jnp.float32) for shape in ((n, 2 * n), (128, 256), (128, 2 * n))]


VMEM = pl.BlockSpec(memory_space=pltpu.VMEM)
SMEM = pl.BlockSpec(memory_space=pltpu.SMEM)


def factor_call(kernel, ins, outs, n, extra=()):
    return pl.pallas_call(
        kernel,
        in_specs=ins,
        out_specs=[VMEM] * len(outs),
        out_shape=[jax.ShapeDtypeStruct(shape, jnp.float32) for shape in outs],
        scratch_shapes=[*extra, *factor_scratch(n)],
        compiler_params=pltpu.CompilerParams(vmem_limit_bytes=24 * 2**20),
        cost_estimate=pl.CostEstimate(flops=6 * 10**9 // len(outs), transcendentals=n, bytes_accessed=8 * n * n),
    )


def inverse_factor(pieces, place, scale):
    n = pieces.shape[-1]
    return factor_call(functools.partial(inverse_kernel, scale), [SMEM, VMEM], [(n, n)], n)(place, pieces)[0]


def inverse_upper(pieces, place, scale):
    n = pieces.shape[-1]
    outs = [(n // 2, n), (n // 2, 2 * n)]
    extra = [pltpu.VMEM((n, n), jnp.float32)]
    return factor_call(functools.partial(upper_kernel, scale), [SMEM, VMEM], outs, n, extra)(place, pieces)


def inverse_lower(top, rest):
    n = top.shape[-1]
    return factor_call(lower_kernel, [VMEM, VMEM], [(n, n)], n)(top, rest)[0]


def final_kernel(inverse_ref, cross_ref, block_ref, mapped_ref, basis_ref, projected_ref, residual_ref):
    inverse = inverse_ref[...]
    projected_ref[...] = dot(dot(inverse, cross_ref[...]), inverse, 1, 1)
    basis_ref[...] = dot(block_ref[...], inverse, 1, 1)
    residual_ref[...] = dot(mapped_ref[...], inverse, 1, 1) - dot(basis_ref[...], projected_ref[...])


def final_results(inverse, cross, block, mapped):
    n = cross.shape[0]
    vmem = pl.BlockSpec(memory_space=pltpu.VMEM)
    return pl.pallas_call(
        final_kernel,
        in_specs=[vmem] * 4,
        out_specs=[vmem] * 3,
        out_shape=[jax.ShapeDtypeStruct(a.shape, jnp.float32) for a in (block, cross, block)],
        compiler_params=pltpu.CompilerParams(vmem_limit_bytes=24 * 2**20),
        cost_estimate=pl.CostEstimate(flops=2 * 10**9, transcendentals=0, bytes_accessed=16 * n * n),
    )(inverse, cross, block, mapped)


def turned(chip):
    return (chip // 4 % 4) * 16 + (chip // 16) * 4 + chip % 4


TURN = [(chip, turned(chip)) for chip in range(64)]


def shards(matrix, start_vectors, interval):
    slab, width = start_vectors.shape
    half = width // 2
    total_rows = slab * 128
    x, k, z, y = (lax.axis_index(a) for a in ALL)
    south = k == 0
    where = jnp.stack([x, k, z, y]).astype(jnp.int32)
    places = jnp.stack([x ^ s for s in range(4)]).astype(jnp.int32)

    orders = (("z", "y"), ("y", "z"))
    indices = (y, z)

    def gather_rows(fours):
        return [gather(v, a).reshape(16 * slab, half) for v, (a, b) in zip(fours, orders)]

    def gather_cols(pair):
        return gather(pair, "x").reshape(8 * slab, half)

    def partial_rows(cols):
        return [dot(plain, cols).reshape(4, 4, slab, half) for plain, across in operator]

    def forward(cols):
        return [full_sum(scatter_sum(v, a), b) for v, (a, b) in zip(partial_rows(cols), orders)]

    def mapped_part(rows):
        (_, first), (_, second) = operator
        return (dot(first, rows[0]) + dot(second, rows[1])).reshape(4, 2 * slab, half)

    def twice_minus(new, old):
        return jax.tree.map(lambda a, b: 2.0 * a - b, new, old)

    def in_order(mine, other, axis):
        return jnp.concatenate([jnp.where(south, mine, other), jnp.where(south, other, mine)], axis=axis)

    def of_half(array, index, axis):
        size = array.shape[axis] // 2
        return lax.dynamic_slice_in_dim(array, index * size, size, axis)

    def gram_part(both):
        side = lax.dynamic_slice_in_dim(both, x * (width // 4), width // 4, 1)
        return dot(side, of_half(both, k, 1), 0, 0)

    received = swap(of_half(start_vectors, 1 - k, 1), "k", 1)
    kept = of_half(start_vectors, k, 1)
    pair = in_order(kept, received, 0)
    pair = lax.ppermute(pair, CHIPS, TURN)

    matrix, received = lax.optimization_barrier((matrix, received))
    other_matrix = swap(matrix, "k", 1)
    pair, first_half = lax.optimization_barrier((pair, prepared(matrix, other_matrix, interval, where, 0)))
    start = [
        by_index(gather(v, b), i) for v, (a, b), i in zip((pair[:slab], pair[slab:]), orders, indices)
    ]
    start[1], where = lax.optimization_barrier((start[1], where))
    operator = [first_half, prepared(matrix, other_matrix, interval, where, 1)]

    first = scatter_sum(mapped_part(gather_rows(start)), "x")
    second = twice_minus(forward(gather_cols(first)), start)
    third = twice_minus(scatter_sum(mapped_part(gather_rows(second)), "x"), first)
    third_cols = gather_cols(third)

    first = forward(third_cols)
    gram = gram_part(in_order(third_cols, swap(third_cols, "k", 1), 1))
    mapped = mapped_part(gather_rows(first))
    _, gram = lax.optimization_barrier((mapped, gram))
    gram = full_sum(gram, "y")
    second = twice_minus(scatter_sum(mapped, "x"), third)
    _, gram = lax.optimization_barrier((second, gram))
    gram = full_sum(gram, "z")
    partial = partial_rows(gather_cols(second))
    _, gram = lax.optimization_barrier((partial[1], gram))
    gram = gather(gram, "x")
    third = [full_sum(scatter_sum(v, a), b) for v, (a, b) in zip(partial, orders)]
    third = twice_minus(third, first)
    gram = in_order(gram, swap(gram, "k", 1), 2)
    mapped = mapped_part(gather_rows(third))

    final = [lax.dynamic_index_in_dim(v, i, 0, keepdims=False) for v, i in zip(third, indices)]
    final = lax.ppermute(jnp.concatenate(final), CHIPS, TURN)
    upper = inverse_upper(gram, places, 1.0 / total_rows)
    final, upper = lax.optimization_barrier((final, upper))
    final = gather_cols(final)
    inverse = inverse_lower(*upper)
    final = dot(in_order(final, swap(final, "k", 1), 1), inverse, 1, 1)
    final_slab = lax.dynamic_slice_in_dim(final, k * slab, slab, 0)

    gram = gather(full_sum(full_sum(gram_part(final), "y"), "z"), "x")
    gram = in_order(gram, swap(gram, "k", 1), 2)
    cross = by_index(dot(final, mapped.reshape(8 * slab, half), 0, 0).reshape(4, -1, half), x)
    mapped, cross = scatter_sum(jnp.stack([mapped.reshape(cross.shape), cross], 1), "x")
    cross = full_sum(full_sum(cross, "y"), "z")
    cross = by_index(gather(cross, "x"), x).reshape(width, half)
    cross = in_order(cross, swap(cross, "k", 1), 1) / total_rows
    mapped_slab = in_order(of_half(mapped, k, 0), swap(of_half(mapped, 1 - k, 0), "k", 1), 1)
    cross, mapped_slab = dot(cross, inverse, 1, 1), dot(mapped_slab, inverse, 1, 1)
    inverse = inverse_factor(gram, places, 1.0 / total_rows)
    return tuple(final_results(inverse, cross, final_slab, mapped_slab))


def solution(mesh):
    torus = Mesh(mesh.devices.reshape(4, 2, 4, 4), ALL)
    placed = (P(ROW, COL), P(COL + ROW, None), P())
    return jax.shard_map(
        shards,
        mesh=torus,
        in_specs=placed,
        out_specs=(P(COL + ROW, None), P(), P(COL + ROW, None)),
        check_vma=False,
    )
```

```python
import functools

import jax
import jax.numpy as jnp
from jax import lax
from jax.experimental import pallas as pl
from jax.experimental.pallas import tpu as pltpu
from jax.sharding import Mesh
from jax.sharding import PartitionSpec as P


ALL = ("x", "k", "z", "y")
CHIPS = ("x", "z", "y")
ROW = ("x", "k")
COL = ("z", "y")


def dot(left, right, left_dim=1, right_dim=0):
    return lax.dot_general(
        left,
        right,
        (((left_dim,), (right_dim,)), ((), ())),
        precision=lax.Precision.HIGHEST,
        preferred_element_type=jnp.float32,
    )


def swap(array, axis, step):
    count = lax.axis_size(axis)
    return lax.ppermute(array, axis, [(i, i ^ step) for i in range(count)])


def scatter_sum(pieces, axis):
    total = pieces[0]
    for step in range(1, pieces.shape[0]):
        total = total + swap(pieces[step], axis, step)
    return total


def gather(piece, axis):
    count = lax.axis_size(axis)
    return jnp.stack([piece] + [swap(piece, axis, step) for step in range(1, count)])


def full_sum(piece, axis):
    terms = [piece] + [swap(piece, axis, step) for step in range(1, lax.axis_size(axis))]
    while len(terms) > 1:
        terms = [a + b for a, b in zip(terms[::2], terms[1::2])]
    return terms[0]


def by_index(pieces, index):
    return jnp.concatenate([lax.dynamic_slice_in_dim(pieces, index ^ s, 1, 0) for s in range(4)])


def slab_at(step, where, half, inner):
    outer, inner = step // 2, 2 * (step % 2) + inner
    if half == 0:
        return (where[2] ^ outer) + 4 * inner
    return inner + 4 * (where[3] ^ outer)


def prepared_kernel(half, where_ref, ends_ref, *refs):
    *piece_refs, out_ref, turned_ref = refs
    x, k, z, y = (where_ref[i] for i in range(4))
    size, width = piece_refs[0].shape
    center = 0.5 * (ends_ref[0] + ends_ref[1])
    half_width = 0.5 * (ends_ref[1] - ends_ref[0])
    first_col = (4 * z + y) * width
    rows = lax.broadcasted_iota(jnp.int32, (size, 128), 0)
    lanes = lax.broadcasted_iota(jnp.int32, (size, 128), 1)
    for inner in range(2):
        slab = slab_at(pl.program_id(0), where_ref, half, inner)
        first_row = x * (32 * size) + slab * (2 * size) + half * size
        mine = slab // 8 == k
        for s in range(4):
            at = pl.multiple_of((x ^ s) * 128, 128)
            own = piece_refs[2 * inner][:, pl.ds(at, 128)]
            other = piece_refs[2 * inner + 1][:, pl.ds(at, 128)]
            values = jnp.where(mine, own, other)
            on = rows + first_row == lanes + (first_col + at)
            values = jnp.where(on, values - center, values) / half_width
            out_ref[size * inner : size * (inner + 1), 128 * s : 128 * (s + 1)] = values
    for s in range(4):
        turned_ref[128 * s : 128 * (s + 1), :] = out_ref[:, 128 * s : 128 * (s + 1)].T


def prepared(own, other, interval, where, half):
    rows, width = own.shape
    size = rows // 16
    pieces = [
        pl.BlockSpec((size, width), lambda i, w, e, n=n: ((2 * slab_at(i, w, half, n) + half) % 16, 0))
        for n in range(2)
    ]
    return pl.pallas_call(
        functools.partial(prepared_kernel, half),
        grid_spec=pltpu.PrefetchScalarGridSpec(
            num_scalar_prefetch=2,
            grid=(8,),
            in_specs=[pieces[0], pieces[0], pieces[1], pieces[1]],
            out_specs=[
                pl.BlockSpec((2 * size, width), lambda i, w, e: (i, 0)),
                pl.BlockSpec((width, 2 * size), lambda i, w, e: (0, i)),
            ],
        ),
        out_shape=[
            jax.ShapeDtypeStruct((rows, width), jnp.float32),
            jax.ShapeDtypeStruct((width, rows), jnp.float32),
        ],
        cost_estimate=pl.CostEstimate(flops=10**9, transcendentals=0, bytes_accessed=16 * rows * width),
    )(where, interval, own, other, own, other)


def panel(aug_ref, p):
    base = 16 * p
    rows = []
    for i in range(16):
        rows.append([
            jnp.broadcast_to(aug_ref[base + i : base + i + 1, :128], (8, 128)),
            jnp.broadcast_to(aug_ref[base + i : base + i + 1, 128:], (8, 128)),
        ])
    splat = {}
    for i in range(16):
        for j in range(i, 16):
            splat[i, j] = jnp.broadcast_to(rows[i][0][:, base + j : base + j + 1], (8, 128))
    for j in range(16):
        inv = lax.rsqrt(splat[j, j])
        u = {}
        for i in range(j + 1, 16):
            u[i] = splat[j, i] * inv
        for a in range(j + 1, 16):
            for b in range(a, 16):
                splat[a, b] = splat[a, b] - u[a] * u[b]
        for t in range(2):
            rows[j][t] = rows[j][t] * inv
        for i in range(j + 1, 16):
            for t in range(2):
                rows[i][t] = rows[i][t] - u[i] * rows[j][t]
    for i in range(16):
        for t in range(2):
            aug_ref[base + i : base + i + 1, 128 * t : 128 * t + 128] = rows[i][t][:1]


def factor_block(aug_ref):
    for p in range(8):
        panel(aug_ref, p)
        if p < 7:
            low = 16 * (p + 1)
            above = aug_ref[:low, :]
            rows = aug_ref[low : low + 16, :]
            aug_ref[low : low + 16, :] = rows - dot(above[:, low : low + 16], above, 0, 0)


def factor_rows(first, last, out_ref, work_ref, aug_ref, done_ref):
    n = work_ref.shape[0]
    rows = lax.broadcasted_iota(jnp.int32, (128, 128), 0)
    lanes = lax.broadcasted_iota(jnp.int32, (128, 128), 1)
    unit = jnp.where(rows == lanes, 1.0, 0.0)

    def step(b, carry):
        at = pl.multiple_of(b * 128, 128)
        aug_ref[:, :128] = work_ref[pl.ds(at, 128), pl.ds(at, 128)]
        aug_ref[:, 128:] = unit
        factor_block(aug_ref)
        done = dot(aug_ref[:, 128:], work_ref[pl.ds(at, 128), :])
        out_ref[pl.ds(at, 128), :] = done[:, n:]
        done_ref[...] = done

        def below(i, carry):
            low = pl.multiple_of(i * 128, 128)
            done = done_ref[...]
            work_ref[pl.ds(low, 128), :] -= dot(done_ref[:, pl.ds(low, 128)], done, 0, 0)
            return carry

        lax.fori_loop(b + 1, n // 128, below, 0)
        return carry

    lax.fori_loop(first, last, step, 0)


def set_up(scale, place_ref, pieces_ref, work_ref):
    count, size, n = pieces_ref.shape
    for i in range(count):
        at = pl.multiple_of(place_ref[i] * size, size)
        work_ref[pl.ds(at, size), :n] = pieces_ref[i] * scale
    rows = lax.broadcasted_iota(jnp.int32, (n, n), 0)
    lanes = lax.broadcasted_iota(jnp.int32, (n, n), 1)
    work_ref[:, n:] = jnp.where(rows == lanes, 1.0, 0.0)


def inverse_kernel(scale, place_ref, pieces_ref, out_ref, work_ref, *scratch):
    set_up(scale, place_ref, pieces_ref, work_ref)
    factor_rows(0, work_ref.shape[0] // 128, out_ref, work_ref, *scratch)


def upper_kernel(scale, place_ref, pieces_ref, out_ref, rest_ref, full_ref, work_ref, *scratch):
    set_up(scale, place_ref, pieces_ref, work_ref)
    top = out_ref.shape[0]
    factor_rows(0, top // 128, full_ref, work_ref, *scratch)
    out_ref[...] = full_ref[:top, :]
    rest_ref[...] = work_ref[top:, :]


def lower_kernel(top_ref, rest_ref, out_ref, work_ref, *scratch):
    top = top_ref.shape[0]
    out_ref[:top, :] = top_ref[...]
    work_ref[top:, :] = rest_ref[...]
    factor_rows(top // 128, work_ref.shape[0] // 128, out_ref, work_ref, *scratch)


def factor_scratch(n):
    return [pltpu.VMEM(shape, jnp.float32) for shape in ((n, 2 * n), (128, 256), (128, 2 * n))]


VMEM = pl.BlockSpec(memory_space=pltpu.VMEM)
SMEM = pl.BlockSpec(memory_space=pltpu.SMEM)


def factor_call(kernel, ins, outs, n, extra=()):
    return pl.pallas_call(
        kernel,
        in_specs=ins,
        out_specs=[VMEM] * len(outs),
        out_shape=[jax.ShapeDtypeStruct(shape, jnp.float32) for shape in outs],
        scratch_shapes=[*extra, *factor_scratch(n)],
        compiler_params=pltpu.CompilerParams(vmem_limit_bytes=24 * 2**20),
        cost_estimate=pl.CostEstimate(flops=6 * 10**9 // len(outs), transcendentals=n, bytes_accessed=8 * n * n),
    )


def inverse_factor(pieces, place, scale):
    n = pieces.shape[-1]
    return factor_call(functools.partial(inverse_kernel, scale), [SMEM, VMEM], [(n, n)], n)(place, pieces)[0]


def inverse_upper(pieces, place, scale):
    n = pieces.shape[-1]
    outs = [(n // 2, n), (n // 2, 2 * n)]
    extra = [pltpu.VMEM((n, n), jnp.float32)]
    return factor_call(functools.partial(upper_kernel, scale), [SMEM, VMEM], outs, n, extra)(place, pieces)


def inverse_lower(top, rest):
    n = top.shape[-1]
    return factor_call(lower_kernel, [VMEM, VMEM], [(n, n)], n)(top, rest)[0]


def final_kernel(inverse_ref, cross_ref, block_ref, mapped_ref, basis_ref, projected_ref, residual_ref):
    inverse = inverse_ref[...]
    projected_ref[...] = dot(dot(inverse, cross_ref[...]), inverse, 1, 1)
    basis_ref[...] = dot(block_ref[...], inverse, 1, 1)
    residual_ref[...] = dot(mapped_ref[...], inverse, 1, 1) - dot(basis_ref[...], projected_ref[...])


def final_results(inverse, cross, block, mapped):
    n = cross.shape[0]
    vmem = pl.BlockSpec(memory_space=pltpu.VMEM)
    return pl.pallas_call(
        final_kernel,
        in_specs=[vmem] * 4,
        out_specs=[vmem] * 3,
        out_shape=[jax.ShapeDtypeStruct(a.shape, jnp.float32) for a in (block, cross, block)],
        compiler_params=pltpu.CompilerParams(vmem_limit_bytes=24 * 2**20),
        cost_estimate=pl.CostEstimate(flops=2 * 10**9, transcendentals=0, bytes_accessed=16 * n * n),
    )(inverse, cross, block, mapped)


def turned(chip):
    return (chip // 4 % 4) * 16 + (chip // 16) * 4 + chip % 4


TURN = [(chip, turned(chip)) for chip in range(64)]


def shards(matrix, start_vectors, interval):
    slab, width = start_vectors.shape
    half = width // 2
    total_rows = slab * 128
    x, k, z, y = (lax.axis_index(a) for a in ALL)
    south = k == 0
    where = jnp.stack([x, k, z, y]).astype(jnp.int32)
    places = jnp.stack([x ^ s for s in range(4)]).astype(jnp.int32)

    orders = (("z", "y"), ("y", "z"))
    indices = (y, z)

    def gather_rows(fours):
        return [gather(v, a).reshape(16 * slab, half) for v, (a, b) in zip(fours, orders)]

    def gather_cols(pair):
        return gather(pair, "x").reshape(8 * slab, half)

    def partial_rows(cols):
        return [dot(plain, cols).reshape(4, 4, slab, half) for plain, across in operator]

    def forward(cols):
        return [full_sum(scatter_sum(v, a), b) for v, (a, b) in zip(partial_rows(cols), orders)]

    def mapped_part(rows):
        (_, first), (_, second) = operator
        return (dot(first, rows[0]) + dot(second, rows[1])).reshape(4, 2 * slab, half)

    def twice_minus(new, old):
        return jax.tree.map(lambda a, b: 2.0 * a - b, new, old)

    def in_order(mine, other, axis):
        return jnp.concatenate([jnp.where(south, mine, other), jnp.where(south, other, mine)], axis=axis)

    def of_half(array, index, axis):
        size = array.shape[axis] // 2
        return lax.dynamic_slice_in_dim(array, index * size, size, axis)

    def gram_part(both):
        side = lax.dynamic_slice_in_dim(both, x * (width // 4), width // 4, 1)
        return dot(side, of_half(both, k, 1), 0, 0)

    received = swap(of_half(start_vectors, 1 - k, 1), "k", 1)
    kept = of_half(start_vectors, k, 1)
    pair = in_order(kept, received, 0)
    pair = lax.ppermute(pair, CHIPS, TURN)

    matrix, received = lax.optimization_barrier((matrix, received))
    other_matrix = swap(matrix, "k", 1)
    pair, first_half = lax.optimization_barrier((pair, prepared(matrix, other_matrix, interval, where, 0)))
    start = [
        by_index(gather(v, b), i) for v, (a, b), i in zip((pair[:slab], pair[slab:]), orders, indices)
    ]
    start[1], where = lax.optimization_barrier((start[1], where))
    operator = [first_half, prepared(matrix, other_matrix, interval, where, 1)]

    first = scatter_sum(mapped_part(gather_rows(start)), "x")
    second = twice_minus(forward(gather_cols(first)), start)
    third = twice_minus(scatter_sum(mapped_part(gather_rows(second)), "x"), first)
    third_cols = gather_cols(third)

    first = forward(third_cols)
    gram = gram_part(in_order(third_cols, swap(third_cols, "k", 1), 1))
    mapped = mapped_part(gather_rows(first))
    _, gram = lax.optimization_barrier((mapped, gram))
    gram = full_sum(gram, "y")
    second = twice_minus(scatter_sum(mapped, "x"), third)
    _, gram = lax.optimization_barrier((second, gram))
    gram = full_sum(gram, "z")
    partial = partial_rows(gather_cols(second))
    _, gram = lax.optimization_barrier((partial[1], gram))
    gram = gather(gram, "x")
    third = [full_sum(scatter_sum(v, a), b) for v, (a, b) in zip(partial, orders)]
    third = twice_minus(third, first)
    gram = in_order(gram, swap(gram, "k", 1), 2)
    mapped = mapped_part(gather_rows(third))

    final = [lax.dynamic_index_in_dim(v, i, 0, keepdims=False) for v, i in zip(third, indices)]
    final = lax.ppermute(jnp.concatenate(final), CHIPS, TURN)
    upper = inverse_upper(gram, places, 1.0 / total_rows)
    final, upper = lax.optimization_barrier((final, upper))
    final = gather_cols(final)
    inverse = inverse_lower(*upper)
    final = dot(in_order(final, swap(final, "k", 1), 1), inverse, 1, 1)
    final_slab = lax.dynamic_slice_in_dim(final, k * slab, slab, 0)

    gram = full_sum(gram_part(final), "y")
    cross = by_index(dot(final, mapped.reshape(8 * slab, half), 0, 0).reshape(4, -1, half), x)
    mapped = jnp.stack([mapped.reshape(cross.shape), cross], 1)
    gram = full_sum(gram, "z")
    mapped, cross = scatter_sum(mapped, "x")
    gram = gather(gram, "x")
    cross = full_sum(cross, "y")
    gram = in_order(gram, swap(gram, "k", 1), 2)
    upper = inverse_upper(gram, places, 1.0 / total_rows)
    cross = full_sum(cross, "z")
    _, upper = lax.optimization_barrier((cross, upper))
    cross = by_index(gather(cross, "x"), x).reshape(width, half)
    mapped_slab = in_order(of_half(mapped, k, 0), swap(of_half(mapped, 1 - k, 0), "k", 1), 1)
    mapped_slab = dot(mapped_slab, inverse, 1, 1)
    first_inverse, inverse = inverse, inverse_lower(*upper)
    cross = in_order(cross, swap(cross, "k", 1), 1) / total_rows
    cross = dot(cross, first_inverse, 1, 1)
    return tuple(final_results(inverse, cross, final_slab, mapped_slab))


def solution(mesh):
    torus = Mesh(mesh.devices.reshape(4, 2, 4, 4), ALL)
    placed = (P(ROW, COL), P(COL + ROW, None), P())
    return jax.shard_map(
        shards,
        mesh=torus,
        in_specs=placed,
        out_specs=(P(COL + ROW, None), P(), P(COL + ROW, None)),
        check_vma=False,
    )
```
